128 devices in a mesh: band: 32 (over z, y, x_hi), grid: 4 (over x_lo, core).
Axes of the slice: x: 4 (x_hi: 2, x_lo: 2; x = x_hi * 2 + x_lo), y: 4, z: 4, core: 2. Of those that a mesh axis runs over, the one named last changes fastest.
Arguments:
- orbitals: float32 [128, 110592], P('band', 'grid'), may hold values from -6 to 6
Outputs:
- exchange_vectors: float32 [128, 110592], P('band', 'grid')
- margin: float32 [128, 128], P('grid', 'band')
The draws below stay inside these ranges and needn't reach their ends.
All inputs are finite; a program needn't handle non-finite values.
Results may differ from the reference program's by a relative error of at most 0.00012.
Values sent between devices are 32-bit elements; how exact they have to be, the bound alone decides.
A program may use at most 128 MiB of HBM per device.

```python
import jax
import jax.numpy as jnp
from jax import lax

NG = 48
BAND_DEV = 4
NBANDS = 128
NCELL = 110592
N_BAND = 32


def steps_of(rng, dims, split, least, top_value):
    gain, own = 1.0, jax.random.fold_in(rng, 6)
    for position, shards_of in split:
        heights = jnp.exp(jax.random.uniform(jax.random.fold_in(own, position), (shards_of,), jnp.float32, least / len(split), top_value / len(split)))
        gain = gain * jnp.repeat(heights, dims[position] // shards_of).reshape([-1 if axis == position else 1 for axis in range(len(dims))])
    return gain


def normal_values(stream_key, shape, deviation, reach, split=(), kind=jnp.bfloat16):
    result = jax.random.normal(stream_key, shape, jnp.float32) * deviation
    if len(split) > 0:
        result = steps_of(stream_key, shape, split, -0.22, 0.18) * result
    return jnp.clip(result, min=-reach, max=reach).astype(kind)


def setup_inputs(seed: int = 0) -> dict:
    streams_of = jax.random.split(jax.random.key(seed), 2)
    orbitals = normal_values(streams_of[0], (NBANDS, NCELL), 1.0, 6.0, ((0, 32), (1, 4)), jnp.float32)
    return dict(orbitals=orbitals)


def folded_freq(count):
    indices = jnp.arange(count)
    return ((indices + count // 2) % count - count // 2).astype(jnp.float32)


def kernel_table():
    freqs = folded_freq(NG)
    squares = freqs[:, None, None] ** 2 + freqs[None, :, None] ** 2 + freqs[None, None, :] ** 2
    safe_sq = jnp.where(squares > 0, squares, jnp.float32(1.0))
    return jnp.where(squares > 0, 40.0 * (1.0 - jnp.exp(-squares / 16.0)) / safe_sq, jnp.float32(0.0))


def reference(orbitals):
    kernel = kernel_table()
    blocks = orbitals.reshape(N_BAND, BAND_DEV, NCELL)
    window = jnp.concatenate([blocks, jnp.roll(blocks, 1, axis=0), jnp.roll(blocks, -1, axis=0)], axis=1)

    def per_band(single, partners):
        density = (single[None, :] * partners).reshape(-1, NG, NG, NG)
        spectrum = jnp.fft.fftn(density, axes=(1, 2, 3))
        potential = jnp.real(jnp.fft.ifftn(spectrum * kernel, axes=(1, 2, 3))).reshape(-1, NCELL)
        return -jnp.sum(partners * potential, axis=0)

    def per_block(args):
        own_block, partners = args
        return lax.map(lambda single: per_band(single, partners), own_block)

    vectors = lax.map(per_block, (blocks, window)).reshape(NBANDS, NCELL).astype(jnp.float32)
    margin = jnp.dot(orbitals, vectors.T, precision=lax.Precision.HIGHEST, preferred_element_type=jnp.float32) / NCELL
    return vectors, margin
```

```python
import functools

import jax
import jax.numpy as jnp
import numpy as np
from jax import lax
from jax.experimental import pallas as pl
from jax.experimental.pallas import tpu as pltpu
from jax.sharding import PartitionSpec as P


def kernel_values(ng):
    freqs = ((np.arange(ng) + ng // 2) % ng - ng // 2).astype(np.float32)
    sq = freqs[: ng // 2 + 1, None, None] ** 2 + freqs[None, :, None] ** 2 + freqs[None, None, :] ** 2
    safe = np.where(sq > 0, sq, np.float32(1.0))
    return np.where(sq > 0, 40.0 * (1.0 - np.exp(-sq / 16.0)) / safe, 0.0)


def hartley(ng):
    k = np.arange(ng)
    ang = (k[:, None] * k[None, :] % ng) * (2.0 * np.pi / ng)
    return np.cos(ang) + np.sin(ang)


def split_const(table):
    table = np.asarray(table, np.float32)
    hi = table.astype(jnp.bfloat16)
    lo = (table - hi.astype(np.float32)).astype(jnp.bfloat16)
    return hi, lo


def rfft(xs):
    n = len(xs)
    if n == 3:
        s = xs[1] + xs[2]
        d = xs[1] - xs[2]
        return [(xs[0] + s, None), (xs[0] - 0.5 * s, d * (-np.sqrt(3.0) / 2))]
    even, odd = rfft(xs[0::2]), rfft(xs[1::2])
    half = n // 2
    out = [None] * (half + 1)
    for k in range(half // 2 + 1):
        er, ei = even[k]
        orr, oi = odd[k]
        if k == 0:
            out[0] = (er + orr, None)
            out[half] = (er - orr, None)
            continue
        c, s = np.cos(2 * np.pi * k / n), -np.sin(2 * np.pi * k / n)
        if 2 * k == half:
            out[k] = (er, -orr)
            continue
        tr, ti = cmul(orr, oi, c, s)
        out[k] = (er + tr, addo(ei, ti))
        out[half - k] = (er - tr, subo(ti, ei))
    return out


def addo(a, b):
    return b if a is None else a + b


def subo(a, b):
    return a if b is None else a - b


def cmul(r, i, c, s):
    if i is None:
        return r * c, r * s
    if abs(abs(c) - abs(s)) < 1e-9:
        if s < 0 < c:
            return (r + i) * c, (i - r) * c
        return (r - i) * c, (r + i) * c
    return r * c - i * s, r * s + i * c


def irfft(spec, n):
    if n == 3:
        dc, (r, i) = spec[0][0], spec[1]
        base = dc - r
        t = i * np.sqrt(3.0)
        return [dc + 2.0 * r, base - t, base + t]
    half = n // 2
    even, odd = [None] * (half // 2 + 1), [None] * (half // 2 + 1)
    for k in range(half // 2 + 1):
        yr, yi = spec[k]
        if k == 0:
            hr = spec[half][0]
            even[0] = (yr + hr, None)
            odd[0] = (yr - hr, None)
            continue
        if 2 * k == half:
            even[k] = (yr + yr, None)
            odd[k] = (-(yi + yi), None)
            continue
        zr, zi = spec[half - k]
        er, ei = yr + zr, yi - zi
        dr, di = yr - zr, yi + zi
        c, s = np.cos(2 * np.pi * k / n), np.sin(2 * np.pi * k / n)
        even[k] = (er, ei)
        odd[k] = cmul(dr, di, c, s)
    ev, od = irfft(even, half), irfft(odd, half)
    out = [None] * n
    out[0::2], out[1::2] = ev, od
    return out


def split(v):
    hi = v.astype(jnp.bfloat16)
    lo = (v - hi.astype(jnp.float32)).astype(jnp.bfloat16)
    return hi, lo


def mm(a, b):
    return jnp.dot(a, b, preferred_element_type=jnp.float32)


def solve_kernel(ng, own_ref, k1_ref, k2_ref, zh_ref, zl_ref, ty_ref, sel_ref, s_ref, o_ref,
                 buf, amp, acc, work, vec, recv, rsem, ssem, nsem, osem, orsem, lsem):
    planes, _, width = own_ref.shape
    me = lax.axis_index("grid")
    band, nband = lax.axis_index("band"), lax.axis_size("band")
    chip, core = me // 2, me % 2
    sib = chip * 2 + (1 - core)
    cross = (1 - chip) * 2 + core
    far = (1 - chip) * 2 + (1 - core)
    above, below = (band + 1) % nband, (band + nband - 1) % nband
    mesh_id = pl.DeviceIdType.MESH

    def remote(src, dst, send, recv_sem, device):
        return pltpu.make_async_remote_copy(
            src_ref=src, dst_ref=dst, send_sem=send, recv_sem=recv_sem,
            device_id=device, device_id_type=mesh_id,
        )

    def share(blk, lane, slot, src, target):
        return remote(src, buf.at[blk, slot], ssem.at[blk, lane], rsem.at[blk, slot], (band, target))

    barrier = pltpu.get_barrier_semaphore()
    for device in ((band, sib), (band, cross), (band, far), (above, cross), (below, cross)):
        pl.semaphore_signal(barrier, inc=1, device_id=device, device_id_type=mesh_id)
    pl.semaphore_wait(barrier, 5)

    share(0, 1, me, own_ref, cross).start()
    share(0, 0, me, own_ref, sib).start()
    remote(own_ref, buf.at[1, me], nsem.at[0], rsem.at[1, me], (above, cross)).start()
    remote(own_ref, buf.at[2, me], nsem.at[1], rsem.at[2, me], (below, cross)).start()
    local = pltpu.make_async_copy(own_ref, buf.at[0, me], lsem)
    local.start()

    def arrived(blk, slot):
        share(blk, 0, slot, own_ref, sib).wait_recv()

    def relay(blk, slot):
        arrived(blk, slot)
        share(blk, 2, slot, buf.at[blk, slot], sib).start()

    def spread(blk):
        arrived(blk, cross)
        share(blk, 1, cross, buf.at[blk, cross], cross).start()
        share(blk, 0, cross, buf.at[blk, cross], sib).start()

    def ztrans(v):
        hi, lo = split(v)
        return mm(hi, zh_ref[...]) + mm(lo, zh_ref[...]) + mm(hi, zl_ref[...])

    def ytrans(v):
        hi, lo = split(v)
        return mm(ty_ref[...], jnp.concatenate([hi, lo, hi], axis=0))

    def slot_of(blk, s):
        turn = s // 2 + jnp.minimum(blk, 1)
        return ((chip + turn) % 2) * 2 + (core + s % 2) % 2

    def amplitude(slot):
        hi, lo = split(buf[0, slot].reshape(planes * ng, width))
        amp[slot] = (mm(hi, sel_ref[me]) + mm(lo, sel_ref[me])).reshape(planes, ng, width)

    def forward(blk, s):
        slot = slot_of(blk, s)

        @pl.when(jnp.logical_and(blk == 0, s == 2))
        def _():
            relay(0, cross)
            spread(1)

        @pl.when(jnp.logical_and(blk == 1, s == 2))
        def _():
            relay(1, me)
            spread(2)

        @pl.when(jnp.logical_and(blk == 2, s == 2))
        def _():
            relay(2, me)

        @pl.when(s % 2 == 1)
        def _():
            arrived(blk, slot)

        @pl.when(blk == 0)
        def _():
            amplitude(slot)

        p = (amp[slot] * buf[blk, slot]).reshape(planes * ng, width)
        q = ztrans(p).reshape(planes, ng, width)
        for r in range(planes):
            work[slot, r] = ytrans(q[r])

    def conv(vals, kern):
        spec = rfft(vals)
        out = []
        for k, (re, im) in enumerate(spec):
            kv = kern(k)
            out.append((re * kv, None if im is None else im * kv))
        return irfft(out, ng)

    def xconv(t):
        order = [(g, h, r) for g in range(4) for h in range(2) for r in range(planes)]
        for i in range(2):
            rows = pl.ds(pl.multiple_of(t * 16 + 8 * i, 8), 8)
            res = conv([work[g, r, rows, h * 128:h * 128 + 128] for g, h, r in order],
                       lambda k: k1_ref[k, rows, :])
            for (g, h, r), v in zip(order, res):
                work[g, r, rows, h * 128:h * 128 + 128] = v
        ra = pl.ds(pl.multiple_of(t * 16, 8), 8)
        rb = pl.ds(pl.multiple_of(t * 16 + 8, 8), 8)
        left = lax.broadcasted_iota(jnp.int32, (8, 128), 1) < 64

        def half(g, h, r):
            u, w = work[g, r, ra, 256:384], work[g, r, rb, 256:384]
            if h == 0:
                return jnp.where(left, u, pltpu.roll(w, 64, 1))
            return jnp.where(left, pltpu.roll(u, 64, 1), w)

        rk = pl.ds(pl.multiple_of(t * 8, 8), 8)
        res = dict(zip(order, conv([half(*o) for o in order], lambda k: k2_ref[k, rk, :])))
        for g in range(4):
            for r in range(planes):
                a, b = res[(g, 0, r)], res[(g, 1, r)]
                work[g, r, ra, 256:384] = jnp.where(left, a, pltpu.roll(b, 64, 1))
                work[g, r, rb, 256:384] = jnp.where(left, pltpu.roll(a, 64, 1), b)

    def push(slot):
        return remote(vec.at[slot], recv.at[me], osem.at[slot], orsem.at[me], (band, slot))

    def inverse(blk, s):
        slot = ((chip + 1 - s // 2) % 2) * 2 + (core + s % 2 + s // 2) % 2
        q = jnp.concatenate([ytrans(work[slot, r]) for r in range(planes)], axis=0)
        w = ztrans(q).reshape(planes, ng, width) * buf[blk, slot]

        @pl.when(blk == 0)
        def _():
            acc[slot] = w

        @pl.when(blk == 1)
        def _():
            acc[slot] += w

        @pl.when(blk == 2)
        def _():
            hi, lo = split((acc[slot] + w).reshape(planes * ng, width))
            out = -(mm(hi, s_ref[...]) + mm(lo, s_ref[...]))
            vec[slot] = out.reshape(planes, ng, s_ref.shape[-1])

            @pl.when(s < 3)
            def _():
                push(slot).start()

    def block(blk, _):
        @pl.when(blk == 0)
        def _():
            local.wait()

        def fwd(s, _):
            forward(blk, s)
            return 0

        def mid(t, _):
            xconv(t)
            return 0

        def inv(s, _):
            inverse(blk, s)
            return 0

        lax.fori_loop(0, 4, fwd, 0)
        lax.fori_loop(0, ng // 16, mid, 0)
        lax.fori_loop(0, 4, inv, 0)
        return 0

    lax.fori_loop(0, 3, block, 0)

    o_ref[me] = vec[me]
    for slot in (sib, cross, far):
        remote(vec.at[slot], recv.at[slot], osem.at[slot], orsem.at[slot], (band, slot)).wait()
        o_ref[slot] = recv[slot]
    for blk in range(3):
        for lane, target in ((0, sib), (1, cross), (2, sib)):
            share(blk, lane, me, own_ref, target).wait_send()
    remote(own_ref, buf.at[1, me], nsem.at[0], rsem.at[1, me], (above, cross)).wait_send()
    remote(own_ref, buf.at[2, me], nsem.at[1], rsem.at[2, me], (below, cross)).wait_send()


def lane_tables(ng, bands):
    w = bands * ng
    half, bz = [], []
    for lo, hi in ((0, 128), (128, w)):
        for h in range(2):
            half.append(np.full(hi - lo, h))
            bz.append(np.arange(lo, hi))
    half, bz = np.concatenate(half), np.concatenate(bz)
    return half, bz // ng, bz % ng


def solve(own, bands, groups):
    planes, ng, width = own.shape
    half, bnd, zed = lane_tables(ng, bands)
    ht = hartley(ng)
    th, tl = split_const(ht)
    same = (half[:, None] == half[None, :])
    zh, zl = split_const(np.where(same & (bnd[:, None] == bnd[None, :]), ht[zed[:, None], zed[None, :]], 0.0))
    ty = np.concatenate([th, th, tl], axis=1)
    copyz = same & (zed[:, None] == zed[None, :])
    sel = np.stack([copyz & (bnd[:, None] == g) for g in range(groups)]).astype(np.float32)
    s = np.zeros((width, 128), np.float32)
    s[np.arange(width), half * ng + zed] = 1.0
    kv = kernel_values(ng).astype(np.float32) / np.float32(ng**3)
    kb = np.tile(kv, (1, 1, bands))
    k1 = kb[:, :, :128]
    rest = kb[:, :, 128:].reshape(kb.shape[0], ng // 16, 2, 8, 64)
    k2 = np.concatenate([rest[:, :, 0], rest[:, :, 1]], axis=-1).reshape(kb.shape[0], ng // 2, 128)
    consts = [k1, k2, zh, zl, ty, sel.astype(jnp.bfloat16), s.astype(jnp.bfloat16)]
    full = (groups, planes, ng, width)
    f32, dma = jnp.float32, pltpu.SemaphoreType.DMA
    return pl.pallas_call(
        functools.partial(solve_kernel, ng),
        out_shape=jax.ShapeDtypeStruct((groups, planes, ng, 128), f32),
        in_specs=[pl.BlockSpec(memory_space=pltpu.VMEM)] * 8,
        out_specs=pl.BlockSpec(memory_space=pltpu.VMEM),
        scratch_shapes=[
            pltpu.VMEM((3,) + full, f32), pltpu.VMEM(full, f32), pltpu.VMEM(full, f32), pltpu.VMEM(full, f32),
            pltpu.VMEM((groups, planes, ng, 128), f32), pltpu.VMEM((groups, planes, ng, 128), f32),
            dma((3, groups)), dma((3, 3)), dma((2,)), dma((groups,)), dma((groups,)), dma(()),
        ],
        compiler_params=pltpu.CompilerParams(
            vmem_limit_bytes=56 * 1024 * 1024, collective_id=0, has_side_effects=True
        ),
        cost_estimate=pl.CostEstimate(flops=10**11, bytes_accessed=10**7, transcendentals=0),
        name="solve",
    )(own, *[jnp.asarray(c) for c in consts])


def margin_kernel(count, size, orb_ref, vec_ref, o_ref, ro, rv, xo, xv, gs, gr, ps, pr,
                  so, sv, qo, qv, sg, qg, sp, qp):
    bands, ncell = orb_ref.shape[0], orb_ref.shape[1] * lax.axis_size("grid")
    me, band, nband = lax.axis_index("grid"), lax.axis_index("band"), lax.axis_size("band")
    chip, core = me // 2, me % 2
    sib = chip * 2 + (1 - core)
    cross = (1 - chip) * 2 + core
    far = (1 - chip) * 2 + (1 - core)
    mesh_id = pl.DeviceIdType.MESH

    def remote(src, dst, send, recv_sem, device):
        return pltpu.make_async_remote_copy(
            src_ref=src, dst_ref=dst, send_sem=send, recv_sem=recv_sem,
            device_id=device, device_id_type=mesh_id,
        )

    def each(n, body):
        def step(k, _):
            body(k)
            return 0

        lax.fori_loop(0, n, step, 0)

    barrier = pltpu.get_barrier_semaphore()
    each(nband, lambda b: pl.semaphore_signal(barrier, inc=1, device_id=(b, cross), device_id_type=mesh_id))
    for other in (sib, far):
        pl.semaphore_signal(barrier, inc=1, device_id=(band, other), device_id_type=mesh_id)
    pl.semaphore_wait(barrier, nband + 2)

    def part(src, dst, send, recv_sem, c):
        cells = pl.ds(pl.multiple_of(c * size, 128), size)
        return remote(src.at[:, cells], dst.at[band], send.at[c], recv_sem.at[band], (c, cross))

    def target(k):
        return (band + k) % count

    each(count, lambda k: part(orb_ref, ro, so, qo, target(k)).start())
    each(count, lambda k: part(vec_ref, rv, sv, qv, target(k)).start())

    def term(b):
        return remote(gs.at[b], gr.at[band], sg.at[b], qg.at[band], (b, cross))

    @pl.when(band < count)
    def _():
        def take(src, dst, x, send, recv_sem):
            def body(b):
                cells = pl.ds(0, size)
                remote(src.at[:, cells], dst.at[b], send.at[0], recv_sem.at[b], (b, cross)).wait_recv()

            each(nband, body)

            def rows(k):
                for h in range(2):
                    x[k, 4 * h : 4 * h + 4, :] = dst[2 * k + h]

            each(nband // 2, rows)
            return split(x[...].reshape(nband * bands, size))

        oh, ol = take(orb_ref, ro, xo, so, qo)
        vh, vl = take(vec_ref, rv, xv, sv, qv)

        def nt(a, b):
            return lax.dot_general(a, b, (((1,), (1,)), ((), ())), preferred_element_type=jnp.float32)

        g = nt(vh, oh) + nt(vh, ol) + nt(vl, oh)
        for b in range(nband):
            gs[b] = g[4 * b : 4 * b + 4]
        each(nband, lambda k: term((band + k) % nband).start())

    def gather(c):
        remote(gs.at[0], gr.at[c], sg.at[0], qg.at[c], (c, cross)).wait_recv()

    each(count, gather)
    total = gr[0]
    for c in range(1, count):
        total += gr[c]
    ps[...] = total

    def swap(slot):
        return remote(ps, pr.at[me], sp.at[slot], qp.at[me], (band, slot))

    for slot in (cross, far, sib):
        swap(slot).start()
    for slot in (cross, far, sib):
        remote(ps, pr.at[slot], sp.at[slot], qp.at[slot], (band, slot)).wait()
    pr[me] = total
    full = (pr[0] + pr[1]) + (pr[2] + pr[3])
    for k in range(4):
        @pl.when(me == k)
        def _():
            width = o_ref.shape[1]
            o_ref[...] = full[:, k * width : (k + 1) * width] * (1.0 / ncell)

    each(count, lambda k: part(orb_ref, ro, so, qo, k).wait_send())
    each(count, lambda k: part(vec_ref, rv, sv, qv, k).wait_send())

    @pl.when(band < count)
    def _():
        each(nband, lambda k: term(k).wait_send())


def chunking(local, nband):
    tiles = local // 128
    per = next(p for p in range(1, tiles + 1) if tiles % p == 0 and tiles // p <= nband)
    return tiles // per, per * 128


def margin_of(orbitals, vectors):
    bands, local = orbitals.shape
    nband, groups = lax.axis_size("band"), lax.axis_size("grid")
    count, size = chunking(local, nband)
    f32, dma = jnp.float32, pltpu.SemaphoreType.DMA
    out = pl.pallas_call(
        functools.partial(margin_kernel, count, size),
        out_shape=jax.ShapeDtypeStruct((bands, nband * bands // groups), f32),
        in_specs=[pl.BlockSpec(memory_space=pltpu.VMEM)] * 2,
        out_specs=pl.BlockSpec(memory_space=pltpu.VMEM),
        scratch_shapes=[
            pltpu.VMEM((nband, bands, size), f32), pltpu.VMEM((nband, bands, size), f32),
            pltpu.VMEM((nband // 2, 8, size), f32), pltpu.VMEM((nband // 2, 8, size), f32),
            pltpu.VMEM((nband, bands, nband * bands), f32), pltpu.VMEM((count, bands, nband * bands), f32),
            pltpu.VMEM((bands, nband * bands), f32), pltpu.VMEM((groups, bands, nband * bands), f32),
            dma((count,)), dma((count,)), dma((nband,)), dma((nband,)),
            dma((nband,)), dma((count,)), dma((groups,)), dma((groups,)),
        ],
        compiler_params=pltpu.CompilerParams(
            vmem_limit_bytes=24 * 1024 * 1024, collective_id=1, has_side_effects=True
        ),
        cost_estimate=pl.CostEstimate(flops=10**9, bytes_accessed=10**6, transcendentals=0),
        name="margin",
    )(orbitals, vectors)
    return out.T


def on_device(orbitals):
    groups = lax.axis_size("grid")
    bands, local = orbitals.shape
    ncell = local * groups
    ng = round(ncell ** (1 / 3))
    xs = local // (ng * ng)
    planes = xs // 2
    t = orbitals.reshape(bands, 2, planes, ng, ng).transpose(2, 3, 1, 0, 4).reshape(planes, ng, 2, bands * ng)
    own = jnp.concatenate([t[:, :, 0, :128], t[:, :, 1, :128], t[:, :, 0, 128:], t[:, :, 1, 128:]], axis=-1)
    out = solve(own, bands, groups)
    vec = out[..., : 2 * ng].reshape(groups, planes, ng, 2, ng).transpose(0, 3, 1, 2, 4)
    vectors = vec.reshape(bands, local)
    margin = margin_of(orbitals, vectors)
    return (vectors, margin)


def solution(mesh):
    return jax.shard_map(
        on_device,
        mesh=mesh,
        in_specs=(P("band", "grid"),),
        out_specs=(P("band", "grid"), P("grid", "band")),
        check_vma=False,
    )
```

```python
import functools

import jax
import jax.numpy as jnp
import numpy as np
from jax import lax
from jax.experimental import pallas as pl
from jax.experimental.pallas import tpu as pltpu
from jax.sharding import PartitionSpec as P


PTS = 6


def freq_order(ng):
    step = ng // PTS
    low = np.arange(step) * PTS
    out = [low, low + 3]
    for k in (1, 2):
        out += [low + k, ng - low - k]
    return np.concatenate(out)


def kernel_values(ng):
    freqs = ((np.arange(ng) + ng // 2) % ng - ng // 2).astype(np.float32)
    fy = freqs[freq_order(ng)]
    sq = freqs[:, None, None] ** 2 + fy[None, :, None] ** 2 + freqs[None, None, :] ** 2
    safe = np.where(sq > 0, sq, np.float32(1.0))
    return np.where(sq > 0, 40.0 * (1.0 - np.exp(-sq / 16.0)) / safe, 0.0)


def cas(ang):
    return np.cos(ang) + np.sin(ang)


def hartley(ng):
    k = np.arange(ng)
    return cas((k[:, None] * k[None, :] % ng) * (2.0 * np.pi / ng))


def mixers(ng):
    step = ng // PTS
    s, k2 = np.arange(step)[:, None], np.arange(step)[None, :]
    out = []
    for k1 in (0, 3, 1, 2):
        ang = s * (k1 + PTS * k2) * (2.0 * np.pi / ng)
        p, m = cas(ang), cas(-ang)
        out.append(p if k1 in (0, 3) else np.block([[p, m], [m, -p]]))
    return out


def mixer_rows(ng):
    step = ng // PTS
    fwd, inv = [], []
    for mat in mixers(ng):
        for rows, keep in ((mat, fwd), (mat.T, inv)):
            wide = np.zeros((rows.shape[0], 2 * step))
            wide[:, : rows.shape[1]] = rows
            keep.append(np.repeat(wide, ng, axis=1))
    return np.stack([np.concatenate(fwd), np.concatenate(inv)])


def split_const(table):
    table = np.asarray(table, np.float32)
    hi = table.astype(jnp.bfloat16)
    lo = (table - hi.astype(np.float32)).astype(jnp.bfloat16)
    return hi, lo


def split(v):
    hi = v.astype(jnp.bfloat16)
    lo = (v - hi.astype(jnp.float32)).astype(jnp.bfloat16)
    return hi, lo


def mm(a, b):
    return jnp.dot(a, b, preferred_element_type=jnp.float32)


def solve_kernel(ng, own_ref, kt_ref, hz_ref, mix_ref, xh_ref, xl_ref, o_ref,
                 buf, amp, acc, ch, cl, zh, zl, cb, wh, wl, kx, vec, recv,
                 rsem, ssem, nsem, osem, orsem, lsem):
    pts, rows, width = own_ref.shape
    bands, step = 4, ng // PTS
    xs = rows // bands
    total = pts * width
    me = lax.axis_index("grid")
    band, nband = lax.axis_index("band"), lax.axis_size("band")
    chip, core = me // 2, me % 2
    sib = chip * 2 + (1 - core)
    cross = (1 - chip) * 2 + core
    far = (1 - chip) * 2 + (1 - core)
    above, below = (band + 1) % nband, (band + nband - 1) % nband
    mesh_id = pl.DeviceIdType.MESH
    root = np.float32(np.sqrt(0.75))

    def remote(src, dst, send, recv_sem, device):
        return pltpu.make_async_remote_copy(
            src_ref=src, dst_ref=dst, send_sem=send, recv_sem=recv_sem,
            device_id=device, device_id_type=mesh_id,
        )

    def share(blk, lane, slot, src, target):
        return remote(src, buf.at[blk, slot], ssem.at[blk, lane], rsem.at[blk, slot], (band, target))

    def each(n, body):
        def one(k, _):
            body(k)
            return 0

        lax.fori_loop(0, n, one, 0)

    barrier = pltpu.get_barrier_semaphore()
    for device in ((band, sib), (band, cross), (band, far), (above, cross), (below, cross)):
        pl.semaphore_signal(barrier, inc=1, device_id=device, device_id_type=mesh_id)
    pl.semaphore_wait(barrier, 5)

    share(0, 1, me, own_ref, cross).start()
    share(0, 0, me, own_ref, sib).start()
    remote(own_ref, buf.at[1, me], nsem.at[0], rsem.at[1, me], (above, cross)).start()
    remote(own_ref, buf.at[2, me], nsem.at[1], rsem.at[2, me], (below, cross)).start()
    local = pltpu.make_async_copy(own_ref, buf.at[0, me], lsem)
    local.start()

    def weights(first, last, cols):
        def one(u, _):
            at = pl.ds(pl.multiple_of(u * ng, 16), ng)
            for d in range(2):
                hi, lo = split(hz_ref[:, :cols] * mix_ref[d, pl.ds(u, 1), :cols])
                wh[d, at, :cols] = hi
                wl[d, at, :cols] = lo
            return 0

        lax.fori_loop(first, last, one, 0)

    weights(0, 2 * step, width)
    weights(2 * step, PTS * step, 2 * width)

    def spread_rows(t):
        upper = lax.broadcasted_iota(jnp.int32, (8, total), 0) < 4
        a = jnp.broadcast_to(kt_ref[pl.ds(2 * t, 1), :], (8, total))
        b = jnp.broadcast_to(kt_ref[pl.ds(2 * t + 1, 1), :], (8, total))
        kx[pl.ds(pl.multiple_of(8 * t, 8), 8), :] = jnp.where(upper, a, b)

    each(ng // 2, spread_rows)

    def arrived(blk, slot):
        share(blk, 0, slot, own_ref, sib).wait_recv()

    def relay(blk, slot):
        arrived(blk, slot)
        share(blk, 2, slot, buf.at[blk, slot], sib).start()

    def spread(blk):
        arrived(blk, cross)
        share(blk, 1, cross, buf.at[blk, cross], cross).start()
        share(blk, 0, cross, buf.at[blk, cross], sib).start()

    def slot_of(blk, s):
        turn = s // 2 + jnp.minimum(blk, 1)
        return ((chip + turn) % 2) * 2 + (core + s % 2) % 2

    def amplitude(slot):
        sub = lax.broadcasted_iota(jnp.int32, (8, 128), 0)
        pick = sub // bands * bands + me

        def one(r):
            for q in range(rows // 8):
                for j in range(width // 128):
                    at = (slot, r, pl.ds(8 * q, 8), pl.ds(128 * j, 128))
                    amp[at] = jnp.take_along_axis(buf[(0,) + at], pick, axis=0)

        each(pts, one)

    def pieces():
        for q in range(rows // 16):
            for j in range(width // 128):
                yield q, j

    def forward(blk, s):
        slot = slot_of(blk, s)

        @pl.when(jnp.logical_and(blk == 0, s == 2))
        def _():
            relay(0, cross)
            spread(1)

        @pl.when(jnp.logical_and(blk == 1, s == 2))
        def _():
            relay(1, me)
            spread(2)

        @pl.when(jnp.logical_and(blk == 2, s == 2))
        def _():
            relay(2, me)

        @pl.when(s % 2 == 1)
        def _():
            arrived(blk, slot)

        @pl.when(blk == 0)
        def _():
            amplitude(slot)

        for q, j in pieces():
            at = (pl.ds(16 * q, 16), pl.ds(128 * j, 128))
            f = [amp[(slot, r) + at] * buf[(blk, slot, r) + at] for r in range(PTS)]
            sa, sb, sc = f[0] + f[3], f[1] + f[4], f[2] + f[5]
            da, db, dc = f[0] - f[3], f[1] - f[4], f[2] - f[5]
            even, odd = sb + sc, db - dc
            comps = (sa + even, da - odd, da + 0.5 * odd, root * (db + dc), sa - 0.5 * even, root * (sb - sc))
            to = pl.ds(pl.multiple_of(slot * rows + 16 * q, 16), 16)
            for c, v in enumerate(comps):
                hi, lo = split(v)
                ch[to, c * width + 128 * j : c * width + 128 * j + 128] = hi
                cl[to, c * width + 128 * j : c * width + 128 * j + 128] = lo

    groups = ((0, 1), (1, 1), (2, 2), (4, 2))

    def planar(d, ah, al, emit):
        for first, count in groups:
            lo, size = first * width, count * width
            for n in range(0, size, 256):
                w = min(256, size - n)
                a, b = ah[:, lo : lo + size], al[:, lo : lo + size]
                g, h = wh[d, lo : lo + size, n : n + w], wl[d, lo : lo + size, n : n + w]
                emit(lo + n, w, mm(a, g) + mm(b, g) + mm(a, h))

    def keep_split(at, w, v):
        zh[:, at : at + w], zl[:, at : at + w] = split(v)

    def keep(at, w, v):
        cb[:, at : at + w] = v

    def xpass(h, l):
        return mm(xh_ref[...], h) + mm(xh_ref[...], l) + mm(xl_ref[...], h)

    def xconv():
        for n in range(0, total, 256):
            h, l = split(xpass(zh[:, n : n + 256], zl[:, n : n + 256]) * kx[:, n : n + 256])
            zh[:, n : n + 256], zl[:, n : n + 256] = split(xpass(h, l))

    def push(slot):
        return remote(vec.at[slot], recv.at[me], osem.at[slot], orsem.at[me], (band, slot))

    def inverse(blk, s):
        slot = ((chip + 1 - s // 2) % 2) * 2 + (core + s % 2 + s // 2) % 2
        fresh = blk == 0
        for q, j in pieces():
            to = pl.ds(pl.multiple_of(slot * rows + 16 * q, 16), 16)
            c0, c3, c1, s1, c2, s2 = [cb[to, c * width + 128 * j : c * width + 128 * j + 128] for c in range(PTS)]
            ea, eb, oa, ob = c0 - 0.5 * c2, root * s2, c3 - 0.5 * c1, root * s1
            even = (c0 + c2, ea + eb, ea - eb)
            odd = (c3 + c1, ob - oa, oa + ob)
            for r in range(PTS):
                v = even[r % 3] + odd[r % 3] if r < 3 else even[r % 3] - odd[r % 3]
                w = v * buf[blk, slot, r, 16 * q : 16 * q + 16, 128 * j : 128 * j + 128]
                at = (slot, j, pl.ds(rows * r + 16 * q, 16))
                acc[at] = jnp.where(fresh, w, acc[at] + w)

        @pl.when(blk == 2)
        def _():
            for j in range(width // 128):
                t = [acc[slot, j, pl.ds(b, pts * xs, stride=bands), :] for b in range(bands)]
                vec[slot, :, 128 * j : 128 * j + 128] = -((t[0] + t[1]) + (t[2] + t[3]))

            @pl.when(s < 3)
            def _():
                push(slot).start()

    def block(blk):
        @pl.when(blk == 0)
        def _():
            local.wait()

        each(4, lambda s: forward(blk, s))
        planar(0, ch, cl, keep_split)
        xconv()
        planar(1, zh, zl, keep)
        each(4, lambda s: inverse(blk, s))

    each(3, block)

    def place(slot, src):
        for r in range(pts):
            for j in range(width // 128):
                piece = src[xs * r : xs * r + xs, 128 * j : 128 * j + 128]
                o_ref[pl.ds(bands * (width // 128 * r + j) + slot, xs, stride=pts * width // 128 * bands), :] = piece

    recv[me] = vec[me]
    for slot in (sib, cross, far):
        remote(vec.at[slot], recv.at[slot], osem.at[slot], orsem.at[slot], (band, slot)).wait()
    for k in range(4):
        place(k, recv[k])
    for blk in range(3):
        for lane, target in ((0, sib), (1, cross), (2, sib)):
            share(blk, lane, me, own_ref, target).wait_send()
    remote(own_ref, buf.at[1, me], nsem.at[0], rsem.at[1, me], (above, cross)).wait_send()
    remote(own_ref, buf.at[2, me], nsem.at[1], rsem.at[2, me], (below, cross)).wait_send()


def solve(own, bands, groups, ng):
    pts, rows, width = own.shape
    step = ng // PTS
    total = pts * width
    xh, xl = split_const(np.kron(hartley(ng), np.eye(bands)))
    hz = np.tile(hartley(ng), (1, 2 * step)).astype(np.float32)
    kt = (kernel_values(ng).astype(np.float32) / np.float32(ng**3)).reshape(ng, total)
    consts = [kt, hz, mixer_rows(ng).astype(np.float32), xh, xl]
    full = (groups, pts, rows, width)
    f32, bf16, dma = jnp.float32, jnp.bfloat16, pltpu.SemaphoreType.DMA
    tall = groups * rows
    xs = rows // bands
    return pl.pallas_call(
        functools.partial(solve_kernel, ng),
        out_shape=jax.ShapeDtypeStruct((pts * rows * width // 128, 128), f32),
        in_specs=[pl.BlockSpec(memory_space=pltpu.VMEM)] * 6,
        out_specs=pl.BlockSpec(memory_space=pltpu.VMEM),
        scratch_shapes=[
            pltpu.VMEM((3,) + full, f32), pltpu.VMEM(full, f32),
            pltpu.VMEM((groups, width // 128, pts * rows, 128), f32),
            pltpu.VMEM((tall, total), bf16), pltpu.VMEM((tall, total), bf16),
            pltpu.VMEM((tall, total), bf16), pltpu.VMEM((tall, total), bf16),
            pltpu.VMEM((tall, total), f32),
            pltpu.VMEM((2, total, 2 * width), bf16), pltpu.VMEM((2, total, 2 * width), bf16),
            pltpu.VMEM((tall, total), f32),
            pltpu.VMEM((groups, pts * xs, width), f32), pltpu.VMEM((groups, pts * xs, width), f32),
            dma((3, groups)), dma((3, 3)), dma((2,)), dma((groups,)), dma((groups,)), dma(()),
        ],
        compiler_params=pltpu.CompilerParams(
            vmem_limit_bytes=56 * 1024 * 1024, collective_id=0, has_side_effects=True
        ),
        cost_estimate=pl.CostEstimate(flops=10**11, bytes_accessed=10**7, transcendentals=0),
        name="solve",
    )(own, *[jnp.asarray(c) for c in consts])


def margin_kernel(count, size, orb_ref, vec_ref, o_ref, ro, rv, xo, xv, gs, gr, ps, pr,
                  so, sv, qo, qv, sg, qg, sp, qp):
    bands, ncell = orb_ref.shape[0], orb_ref.shape[1] * lax.axis_size("grid")
    me, band, nband = lax.axis_index("grid"), lax.axis_index("band"), lax.axis_size("band")
    chip, core = me // 2, me % 2
    sib = chip * 2 + (1 - core)
    cross = (1 - chip) * 2 + core
    far = (1 - chip) * 2 + (1 - core)
    mesh_id = pl.DeviceIdType.MESH

    def remote(src, dst, send, recv_sem, device):
        return pltpu.make_async_remote_copy(
            src_ref=src, dst_ref=dst, send_sem=send, recv_sem=recv_sem,
            device_id=device, device_id_type=mesh_id,
        )

    def each(n, body):
        def step(k, _):
            body(k)
            return 0

        lax.fori_loop(0, n, step, 0)

    barrier = pltpu.get_barrier_semaphore()
    each(nband, lambda b: pl.semaphore_signal(barrier, inc=1, device_id=(b, cross), device_id_type=mesh_id))
    for other in (sib, far):
        pl.semaphore_signal(barrier, inc=1, device_id=(band, other), device_id_type=mesh_id)
    pl.semaphore_wait(barrier, nband + 2)

    def part(src, dst, send, recv_sem, c):
        cells = pl.ds(pl.multiple_of(c * size, 128), size)
        return remote(src.at[:, cells], dst.at[band], send.at[c], recv_sem.at[band], (c, cross))

    def target(k):
        return (band + k) % count

    each(count, lambda k: part(orb_ref, ro, so, qo, target(k)).start())
    each(count, lambda k: part(vec_ref, rv, sv, qv, target(k)).start())

    def term(b):
        return remote(gs.at[b], gr.at[band], sg.at[b], qg.at[band], (b, cross))

    @pl.when(band < count)
    def _():
        def take(src, dst, x, send, recv_sem):
            def body(b):
                cells = pl.ds(0, size)
                remote(src.at[:, cells], dst.at[b], send.at[0], recv_sem.at[b], (b, cross)).wait_recv()

            each(nband, body)

            def rows(k):
                for h in range(2):
                    x[k, 4 * h : 4 * h + 4, :] = dst[2 * k + h]

            each(nband // 2, rows)
            return split(x[...].reshape(nband * bands, size))

        oh, ol = take(orb_ref, ro, xo, so, qo)
        vh, vl = take(vec_ref, rv, xv, sv, qv)

        def nt(a, b):
            return lax.dot_general(a, b, (((1,), (1,)), ((), ())), preferred_element_type=jnp.float32)

        g = nt(vh, oh) + nt(vh, ol) + nt(vl, oh)
        for b in range(nband):
            gs[b] = g[4 * b : 4 * b + 4]
        each(nband, lambda k: term((band + k) % nband).start())

    def gather(c):
        remote(gs.at[0], gr.at[c], sg.at[0], qg.at[c], (c, cross)).wait_recv()

    each(count, gather)
    total = gr[0]
    for c in range(1, count):
        total += gr[c]
    ps[...] = total

    def swap(slot):
        return remote(ps, pr.at[me], sp.at[slot], qp.at[me], (band, slot))

    for slot in (cross, far, sib):
        swap(slot).start()
    for slot in (cross, far, sib):
        remote(ps, pr.at[slot], sp.at[slot], qp.at[slot], (band, slot)).wait()
    pr[me] = total
    full = (pr[0] + pr[1]) + (pr[2] + pr[3])
    for k in range(4):
        @pl.when(me == k)
        def _():
            width = o_ref.shape[1]
            o_ref[...] = full[:, k * width : (k + 1) * width] * (1.0 / ncell)

    each(count, lambda k: part(orb_ref, ro, so, qo, k).wait_send())
    each(count, lambda k: part(vec_ref, rv, sv, qv, k).wait_send())

    @pl.when(band < count)
    def _():
        each(nband, lambda k: term(k).wait_send())


def chunking(local, nband):
    tiles = local // 128
    per = next(p for p in range(1, tiles + 1) if tiles % p == 0 and tiles // p <= nband)
    return tiles // per, per * 128


def margin_of(orbitals, vectors):
    bands, local = orbitals.shape
    nband, groups = lax.axis_size("band"), lax.axis_size("grid")
    count, size = chunking(local, nband)
    f32, dma = jnp.float32, pltpu.SemaphoreType.DMA
    out = pl.pallas_call(
        functools.partial(margin_kernel, count, size),
        out_shape=jax.ShapeDtypeStruct((bands, nband * bands // groups), f32),
        in_specs=[pl.BlockSpec(memory_space=pltpu.VMEM)] * 2,
        out_specs=pl.BlockSpec(memory_space=pltpu.VMEM),
        scratch_shapes=[
            pltpu.VMEM((nband, bands, size), f32), pltpu.VMEM((nband, bands, size), f32),
            pltpu.VMEM((nband // 2, 8, size), f32), pltpu.VMEM((nband // 2, 8, size), f32),
            pltpu.VMEM((nband, bands, nband * bands), f32), pltpu.VMEM((count, bands, nband * bands), f32),
            pltpu.VMEM((bands, nband * bands), f32), pltpu.VMEM((groups, bands, nband * bands), f32),
            dma((count,)), dma((count,)), dma((nband,)), dma((nband,)),
            dma((nband,)), dma((count,)), dma((groups,)), dma((groups,)),
        ],
        compiler_params=pltpu.CompilerParams(
            vmem_limit_bytes=24 * 1024 * 1024, collective_id=1, has_side_effects=True
        ),
        cost_estimate=pl.CostEstimate(flops=10**9, bytes_accessed=10**6, transcendentals=0),
        name="margin",
    )(orbitals, vectors)
    return out.T


def on_device(orbitals):
    groups = lax.axis_size("grid")
    bands, local = orbitals.shape
    ncell = local * groups
    ng = round(ncell ** (1 / 3))
    xs, wide = local // (ng * ng), ng * ng // PTS
    t = orbitals.reshape(bands, xs, PTS, wide // 128, 128).transpose(2, 1, 0, 3, 4)
    out = solve(t.reshape(PTS, xs * bands, wide), bands, groups, ng)
    vectors = out.reshape(local // 128, bands, 128).transpose(1, 0, 2).reshape(bands, local)
    margin = margin_of(orbitals, vectors)
    return (vectors, margin)


def solution(mesh):
    return jax.shard_map(
        on_device,
        mesh=mesh,
        in_specs=(P("band", "grid"),),
        out_specs=(P("band", "grid"), P("grid", "band")),
        check_vma=False,
    )
```

```python
import functools

import jax
import jax.numpy as jnp
import numpy as np
from jax import lax
from jax.experimental import pallas as pl
from jax.experimental.pallas import tpu as pltpu
from jax.sharding import PartitionSpec as P


PTS = 6


def freq_order(ng):
    step = ng // PTS
    low = np.arange(step) * PTS
    out = [low, low + 3]
    for k in (1, 2):
        out += [low + k, ng - low - k]
    return np.concatenate(out)


def kernel_values(ng):
    freqs = ((np.arange(ng) + ng // 2) % ng - ng // 2).astype(np.float32)
    fy = freqs[freq_order(ng)]
    sq = freqs[:, None, None] ** 2 + fy[None, :, None] ** 2 + freqs[None, None, :] ** 2
    safe = np.where(sq > 0, sq, np.float32(1.0))
    return np.where(sq > 0, 40.0 * (1.0 - np.exp(-sq / 16.0)) / safe, 0.0)


def cas(ang):
    return np.cos(ang) + np.sin(ang)


def hartley(ng):
    k = np.arange(ng)
    return cas((k[:, None] * k[None, :] % ng) * (2.0 * np.pi / ng))


def mixers(ng):
    step = ng // PTS
    s, k2 = np.arange(step)[:, None], np.arange(step)[None, :]
    out = []
    for k1 in (0, 3, 1, 2):
        ang = s * (k1 + PTS * k2) * (2.0 * np.pi / ng)
        p, m = cas(ang), cas(-ang)
        out.append(p if k1 in (0, 3) else np.block([[p, m], [m, -p]]))
    return out


def mixer_rows(ng):
    step = ng // PTS
    fwd, inv = [], []
    for mat in mixers(ng):
        for rows, keep in ((mat, fwd), (mat.T, inv)):
            wide = np.zeros((rows.shape[0], 2 * step))
            wide[:, : rows.shape[1]] = rows
            keep.append(np.repeat(wide, ng, axis=1))
    return np.stack([np.concatenate(fwd), np.concatenate(inv)])


def split_const(table):
    table = np.asarray(table, np.float32)
    hi = table.astype(jnp.bfloat16)
    lo = (table - hi.astype(np.float32)).astype(jnp.bfloat16)
    return hi, lo


def split(v):
    hi = v.astype(jnp.bfloat16)
    lo = (v - hi.astype(jnp.float32)).astype(jnp.bfloat16)
    return hi, lo


def mm(a, b):
    return jnp.dot(a, b, preferred_element_type=jnp.float32)


def solve_kernel(ng, count, orb_ref, kt_ref, hz_ref, mix_ref, xh_ref, xl_ref, o_ref, m_ref,
                 buf, amp, acc, ch, cl, zh, zl, cb, wh, wl, kx, vec, recv,
                 ro, rv, xo, xv, gs, gr, ps, pr,
                 rsem, ssem, nsem, osem, orsem, so, sv, qo, qv, sg, qg, sp, qp):
    pts, rows, width = buf.shape[2:]
    bands, step = 4, ng // PTS
    xs = rows // bands
    total = pts * width
    me = lax.axis_index("grid")
    band, nband = lax.axis_index("band"), lax.axis_size("band")
    chip, core = me // 2, me % 2
    sib = chip * 2 + (1 - core)
    cross = (1 - chip) * 2 + core
    far = (1 - chip) * 2 + (1 - core)
    above, below = (band + 1) % nband, (band + nband - 1) % nband
    mesh_id = pl.DeviceIdType.MESH
    root = np.float32(np.sqrt(0.75))

    def remote(src, dst, send, recv_sem, device):
        return pltpu.make_async_remote_copy(
            src_ref=src, dst_ref=dst, send_sem=send, recv_sem=recv_sem,
            device_id=device, device_id_type=mesh_id,
        )

    def share(blk, lane, slot, src, target):
        return remote(src, buf.at[blk, slot], ssem.at[blk, lane], rsem.at[blk, slot], (band, target))

    def each(n, body):
        def one(k, _):
            body(k)
            return 0

        lax.fori_loop(0, n, one, 0)

    own_ref = buf.at[0, me]

    def lay_own(q):
        for h in range(2):
            for r in range(pts):
                for j in range(width // 128):
                    unit = ((2 * q + h) * pts + r) * (width // 128) + j
                    piece = orb_ref[bands * unit : bands * unit + bands, :]
                    at = (me, r, pl.ds(8 * q + 4 * h, bands), pl.ds(128 * j, 128))
                    buf[(0,) + at] = piece

    for q in range(xs // 2):
        lay_own(q)

    barrier = pltpu.get_barrier_semaphore()
    each(nband, lambda b: pl.semaphore_signal(barrier, inc=1, device_id=(b, cross), device_id_type=mesh_id))
    for other in (sib, far):
        pl.semaphore_signal(barrier, inc=1, device_id=(band, other), device_id_type=mesh_id)
    pl.semaphore_wait(barrier, nband + 2)

    share(0, 1, me, own_ref, cross).start()
    share(0, 0, me, own_ref, sib).start()
    remote(own_ref, buf.at[1, me], nsem.at[0], rsem.at[1, me], (above, cross)).start()
    remote(own_ref, buf.at[2, me], nsem.at[1], rsem.at[2, me], (below, cross)).start()

    def weights(first, last, cols):
        def one(u, _):
            at = pl.ds(pl.multiple_of(u * ng, 16), ng)
            for d in range(2):
                hi, lo = split(hz_ref[:, :cols] * mix_ref[d, pl.ds(u, 1), :cols])
                wh[d, at, :cols] = hi
                wl[d, at, :cols] = lo
            return 0

        lax.fori_loop(first, last, one, 0)

    weights(0, 2 * step, width)
    weights(2 * step, PTS * step, 2 * width)

    def spread_rows(t):
        upper = lax.broadcasted_iota(jnp.int32, (8, total), 0) < 4
        a = jnp.broadcast_to(kt_ref[pl.ds(2 * t, 1), :], (8, total))
        b = jnp.broadcast_to(kt_ref[pl.ds(2 * t + 1, 1), :], (8, total))
        kx[pl.ds(pl.multiple_of(8 * t, 8), 8), :] = jnp.where(upper, a, b)

    each(ng // 2, spread_rows)

    def arrived(blk, slot):
        share(blk, 0, slot, own_ref, sib).wait_recv()

    def relay(blk, slot):
        arrived(blk, slot)
        share(blk, 2, slot, buf.at[blk, slot], sib).start()

    def spread(blk):
        arrived(blk, cross)
        share(blk, 1, cross, buf.at[blk, cross], cross).start()
        share(blk, 0, cross, buf.at[blk, cross], sib).start()

    def slot_of(blk, s):
        turn = s // 2 + jnp.minimum(blk, 1)
        return ((chip + turn) % 2) * 2 + (core + s % 2) % 2

    def amplitude(slot):
        sub = lax.broadcasted_iota(jnp.int32, (8, 128), 0)
        pick = sub // bands * bands + me

        def one(r):
            for q in range(rows // 8):
                for j in range(width // 128):
                    at = (slot, r, pl.ds(8 * q, 8), pl.ds(128 * j, 128))
                    amp[at] = jnp.take_along_axis(buf[(0,) + at], pick, axis=0)

        each(pts, one)

    def pieces():
        for q in range(rows // 16):
            for j in range(width // 128):
                yield q, j

    def forward(blk, s):
        slot = slot_of(blk, s)

        @pl.when(jnp.logical_and(blk == 0, s == 2))
        def _():
            relay(0, cross)
            spread(1)

        @pl.when(jnp.logical_and(blk == 1, s == 2))
        def _():
            relay(1, me)
            spread(2)

        @pl.when(jnp.logical_and(blk == 2, s == 2))
        def _():
            relay(2, me)

        @pl.when(s % 2 == 1)
        def _():
            arrived(blk, slot)

        @pl.when(blk == 0)
        def _():
            amplitude(slot)

        for q, j in pieces():
            at = (pl.ds(16 * q, 16), pl.ds(128 * j, 128))
            f = [amp[(slot, r) + at] * buf[(blk, slot, r) + at] for r in range(PTS)]
            sa, sb, sc = f[0] + f[3], f[1] + f[4], f[2] + f[5]
            da, db, dc = f[0] - f[3], f[1] - f[4], f[2] - f[5]
            even, odd = sb + sc, db - dc
            comps = (sa + even, da - odd, da + 0.5 * odd, root * (db + dc), sa - 0.5 * even, root * (sb - sc))
            to = pl.ds(pl.multiple_of(slot * rows + 16 * q, 16), 16)
            for c, v in enumerate(comps):
                hi, lo = split(v)
                ch[to, c * width + 128 * j : c * width + 128 * j + 128] = hi
                cl[to, c * width + 128 * j : c * width + 128 * j + 128] = lo

    groups = ((0, 1), (1, 1), (2, 2), (4, 2))

    def planar(d, ah, al, emit):
        for first, count in groups:
            lo, size = first * width, count * width
            for n in range(0, size, 256):
                w = min(256, size - n)
                a, b = ah[:, lo : lo + size], al[:, lo : lo + size]
                g, h = wh[d, lo : lo + size, n : n + w], wl[d, lo : lo + size, n : n + w]
                emit(lo + n, w, mm(a, g) + mm(b, g) + mm(a, h))

    def keep_split(at, w, v):
        zh[:, at : at + w], zl[:, at : at + w] = split(v)

    def keep(at, w, v):
        cb[:, at : at + w] = v

    def xpass(h, l):
        return mm(xh_ref[...], h) + mm(xh_ref[...], l) + mm(xl_ref[...], h)

    def xconv():
        for n in range(0, total, 256):
            h, l = split(xpass(zh[:, n : n + 256], zl[:, n : n + 256]) * kx[:, n : n + 256])
            zh[:, n : n + 256], zl[:, n : n + 256] = split(xpass(h, l))

    def push(slot):
        return remote(vec.at[slot], recv.at[me], osem.at[slot], orsem.at[me], (band, slot))

    def inverse(blk, s):
        slot = ((chip + 1 - s // 2) % 2) * 2 + (core + s % 2 + s // 2) % 2
        fresh = blk == 0
        for q, j in pieces():
            to = pl.ds(pl.multiple_of(slot * rows + 16 * q, 16), 16)
            c0, c3, c1, s1, c2, s2 = [cb[to, c * width + 128 * j : c * width + 128 * j + 128] for c in range(PTS)]
            ea, eb, oa, ob = c0 - 0.5 * c2, root * s2, c3 - 0.5 * c1, root * s1
            even = (c0 + c2, ea + eb, ea - eb)
            odd = (c3 + c1, ob - oa, oa + ob)
            for r in range(PTS):
                v = even[r % 3] + odd[r % 3] if r < 3 else even[r % 3] - odd[r % 3]
                w = v * buf[blk, slot, r, 16 * q : 16 * q + 16, 128 * j : 128 * j + 128]
                at = (slot, j, pl.ds(rows * r + 16 * q, 16))
                acc[at] = jnp.where(fresh, w, acc[at] + w)

        @pl.when(blk == 2)
        def _():
            for j in range(width // 128):
                t = [acc[slot, j, pl.ds(b, pts * xs, stride=bands), :] for b in range(bands)]
                vec[slot, :, 128 * j : 128 * j + 128] = -((t[0] + t[1]) + (t[2] + t[3]))

            @pl.when(s < 3)
            def _():
                push(slot).start()

    size = orb_ref.shape[0] // count

    def part(src, dst, send, recv_sem, c):
        cells = pl.ds(pl.multiple_of(c * size, 8), size)
        return remote(src.at[cells], dst.at[band], send.at[c], recv_sem.at[band], (c, cross))

    def target(k):
        return (band + k) % count

    def term(b):
        return remote(gs.at[b], gr.at[band], sg.at[b], qg.at[band], (b, cross))

    def take(src, dst, x, send, recv_sem):
        def body(b):
            remote(src.at[pl.ds(0, size)], dst.at[b], send.at[0], recv_sem.at[b], (b, cross)).wait_recv()

        each(nband, body)

        def lay(k):
            for h in range(2):
                for t in range(size // bands):
                    row = dst[2 * k + h, bands * t : bands * t + bands, :]
                    x[k, 4 * h : 4 * h + 4, 128 * t : 128 * t + 128] = row

        each(nband // 2, lay)

    def nt(a, b):
        return lax.dot_general(a, b, (((1,), (1,)), ((), ())), preferred_element_type=jnp.float32)

    def swap(slot):
        return remote(ps, pr.at[me], sp.at[slot], qp.at[me], (band, slot))

    def margin():
        wide = size // bands * 128

        @pl.when(band < count)
        def _():
            take(orb_ref, ro, xo, so, qo)
            oh, ol = split(xo[...].reshape(nband * bands, wide))
            take(o_ref, rv, xv, sv, qv)
            vh, vl = split(xv[...].reshape(nband * bands, wide))
            g = nt(vh, oh) + nt(vh, ol) + nt(vl, oh)
            for b in range(nband):
                gs[b] = g[4 * b : 4 * b + 4]
            each(nband, lambda k: term((band + k) % nband).start())

        def gather(c):
            remote(gs.at[0], gr.at[c], sg.at[0], qg.at[c], (c, cross)).wait_recv()

        each(count, gather)
        sums = gr[0]
        for c in range(1, count):
            sums += gr[c]
        ps[...] = sums
        for slot in (cross, far, sib):
            swap(slot).start()
        for slot in (cross, far, sib):
            remote(ps, pr.at[slot], sp.at[slot], qp.at[slot], (band, slot)).wait()
        pr[me] = sums
        full = ((pr[0] + pr[1]) + (pr[2] + pr[3])) * (1.0 / ng**3)
        for k in range(4):
            @pl.when(me == k)
            def _():
                m_ref[...] = full[:, k * m_ref.shape[1] : (k + 1) * m_ref.shape[1]]

    def block(blk):
        each(4, lambda s: forward(blk, s))
        planar(0, ch, cl, keep_split)
        xconv()

        @pl.when(blk == 1)
        def _():
            each(count, lambda k: part(orb_ref, ro, so, qo, target(k)).start())

        planar(1, zh, zl, keep)
        each(4, lambda s: inverse(blk, s))

    each(3, block)

    def place(slot, src):
        for r in range(pts):
            for j in range(width // 128):
                piece = src[xs * r : xs * r + xs, 128 * j : 128 * j + 128]
                o_ref[pl.ds(bands * (width // 128 * r + j) + slot, xs, stride=pts * width // 128 * bands), :] = piece

    recv[me] = vec[me]
    for slot in (sib, cross, far):
        remote(vec.at[slot], recv.at[slot], osem.at[slot], orsem.at[slot], (band, slot)).wait()
    for k in range(4):
        place(k, recv[k])
    each(count, lambda k: part(o_ref, rv, sv, qv, target(k)).start())
    margin()
    each(count, lambda k: part(orb_ref, ro, so, qo, k).wait_send())
    each(count, lambda k: part(o_ref, rv, sv, qv, k).wait_send())

    @pl.when(band < count)
    def _():
        each(nband, lambda k: term(k).wait_send())

    for blk in range(3):
        for lane, target in ((0, sib), (1, cross), (2, sib)):
            share(blk, lane, me, own_ref, target).wait_send()
    remote(own_ref, buf.at[1, me], nsem.at[0], rsem.at[1, me], (above, cross)).wait_send()
    remote(own_ref, buf.at[2, me], nsem.at[1], rsem.at[2, me], (below, cross)).wait_send()


def solve(orb, bands, groups, nband, ng):
    width = ng * ng // PTS
    pts, rows = PTS, orb.shape[0] * 128 // (PTS * width)
    step = ng // PTS
    total = pts * width
    xh, xl = split_const(np.kron(hartley(ng), np.eye(bands)))
    hz = np.tile(hartley(ng), (1, 2 * step)).astype(np.float32)
    kt = (kernel_values(ng).astype(np.float32) / np.float32(ng**3)).reshape(ng, total)
    consts = [kt, hz, mixer_rows(ng).astype(np.float32), xh, xl]
    full = (groups, pts, rows, width)
    f32, bf16, dma = jnp.float32, jnp.bfloat16, pltpu.SemaphoreType.DMA
    tall = groups * rows
    xs = rows // bands
    count, wide = chunking(orb.shape[0] * 128 // bands, nband)
    size, nall = wide * bands // 128, nband * bands
    vmem = pl.BlockSpec(memory_space=pltpu.VMEM)
    return pl.pallas_call(
        functools.partial(solve_kernel, ng, count),
        out_shape=[jax.ShapeDtypeStruct(orb.shape, f32), jax.ShapeDtypeStruct((bands, nall // groups), f32)],
        in_specs=[vmem] * 6,
        out_specs=[vmem] * 2,
        scratch_shapes=[
            pltpu.VMEM((3,) + full, f32), pltpu.VMEM(full, f32),
            pltpu.VMEM((groups, width // 128, pts * rows, 128), f32),
            pltpu.VMEM((tall, total), bf16), pltpu.VMEM((tall, total), bf16),
            pltpu.VMEM((tall, total), bf16), pltpu.VMEM((tall, total), bf16),
            pltpu.VMEM((tall, total), f32),
            pltpu.VMEM((2, total, 2 * width), bf16), pltpu.VMEM((2, total, 2 * width), bf16),
            pltpu.VMEM((tall, total), f32),
            pltpu.VMEM((groups, pts * xs, width), f32), pltpu.VMEM((groups, pts * xs, width), f32),
            pltpu.VMEM((nband, size, 128), f32), pltpu.VMEM((nband, size, 128), f32),
            pltpu.VMEM((nband // 2, 8, wide), f32), pltpu.VMEM((nband // 2, 8, wide), f32),
            pltpu.VMEM((nband, bands, nall), f32), pltpu.VMEM((count, bands, nall), f32),
            pltpu.VMEM((bands, nall), f32), pltpu.VMEM((groups, bands, nall), f32),
            dma((3, groups)), dma((3, 3)), dma((2,)), dma((groups,)), dma((groups,)),
            dma((count,)), dma((count,)), dma((nband,)), dma((nband,)),
            dma((nband,)), dma((count,)), dma((groups,)), dma((groups,)),
        ],
        compiler_params=pltpu.CompilerParams(
            vmem_limit_bytes=56 * 1024 * 1024, collective_id=0, has_side_effects=True
        ),
        cost_estimate=pl.CostEstimate(flops=10**11, bytes_accessed=10**7, transcendentals=0),
        name="solve",
    )(orb, *[jnp.asarray(c) for c in consts])


def chunking(local, nband):
    tiles = local // 128
    per = next(p for p in range(1, tiles + 1) if tiles % p == 0 and tiles // p <= nband)
    return tiles // per, per * 128


def on_device(orbitals):
    groups = lax.axis_size("grid")
    bands, local = orbitals.shape
    ncell = local * groups
    ng = round(ncell ** (1 / 3))
    raw = orbitals.reshape(bands, local // 128, 128).transpose(1, 0, 2).reshape(bands * local // 128, 128)
    out, margin = solve(raw, bands, groups, lax.axis_size("band"), ng)
    vectors = out.reshape(local // 128, bands, 128).transpose(1, 0, 2).reshape(bands, local)
    return (vectors, margin.T)


def solution(mesh):
    return jax.shard_map(
        on_device,
        mesh=mesh,
        in_specs=(P("band", "grid"),),
        out_specs=(P("band", "grid"), P("grid", "band")),
        check_vma=False,
    )
```

```python
import functools

import jax
import jax.numpy as jnp
import numpy as np
from jax import lax
from jax.experimental import pallas as pl
from jax.experimental.pallas import tpu as pltpu
from jax.sharding import PartitionSpec as P


PTS = 6


def freq_order(ng):
    step = ng // PTS
    low = np.arange(step) * PTS
    out = [low, low + 3]
    for k in (1, 2):
        out += [low + k, ng - low - k]
    return np.concatenate(out)


def kernel_values(ng):
    freqs = ((np.arange(ng) + ng // 2) % ng - ng // 2).astype(np.float32)
    fy = freqs[freq_order(ng)]
    sq = freqs[:, None, None] ** 2 + fy[None, :, None] ** 2 + freqs[None, None, :] ** 2
    safe = np.where(sq > 0, sq, np.float32(1.0))
    return np.where(sq > 0, 40.0 * (1.0 - np.exp(-sq / 16.0)) / safe, 0.0)


def cas(ang):
    return np.cos(ang) + np.sin(ang)


def hartley(ng):
    k = np.arange(ng)
    return cas((k[:, None] * k[None, :] % ng) * (2.0 * np.pi / ng))


def mixers(ng):
    step = ng // PTS
    s, k2 = np.arange(step)[:, None], np.arange(step)[None, :]
    out = []
    for k1 in (0, 3, 1, 2):
        ang = s * (k1 + PTS * k2) * (2.0 * np.pi / ng)
        p, m = cas(ang), cas(-ang)
        out.append(p if k1 in (0, 3) else np.block([[p, m], [m, -p]]))
    return out


def mixer_rows(ng):
    step = ng // PTS
    fwd, inv = [], []
    for mat in mixers(ng):
        for rows, keep in ((mat, fwd), (mat.T, inv)):
            wide = np.zeros((rows.shape[0], 2 * step))
            wide[:, : rows.shape[1]] = rows
            keep.append(np.repeat(wide, ng, axis=1))
    return np.stack([np.concatenate(fwd), np.concatenate(inv)])


def split_const(table):
    table = np.asarray(table, np.float32)
    hi = table.astype(jnp.bfloat16)
    lo = (table - hi.astype(np.float32)).astype(jnp.bfloat16)
    return hi, lo


def split(v):
    hi = v.astype(jnp.bfloat16)
    lo = (v - hi.astype(jnp.float32)).astype(jnp.bfloat16)
    return hi, lo


def mm(a, b):
    return jnp.dot(a, b, preferred_element_type=jnp.float32)


def solve_kernel(ng, count, orb_ref, kt_ref, hz_ref, mix_ref, xh_ref, xl_ref, o_ref, m_ref,
                 buf, amp, acc, ch, cl, zh, zl, cb, wh, wl, kx, vec, recv,
                 ox, ro, rv, xo, xv, gs, gr, ps, pr,
                 rsem, ssem, nsem, fsem, osem, orsem, so, sv, qo, qv, sg, qg, sp, qp):
    pts, rows, width = buf.shape[2:]
    bands, step = 4, ng // PTS
    xs = rows // bands
    total = pts * width
    me = lax.axis_index("grid")
    band, nband = lax.axis_index("band"), lax.axis_size("band")
    chip, core = me // 2, me % 2
    sib = chip * 2 + (1 - core)
    cross = (1 - chip) * 2 + core
    far = (1 - chip) * 2 + (1 - core)
    above, below = (band + 1) % nband, (band + nband - 1) % nband
    mesh_id = pl.DeviceIdType.MESH
    root = np.float32(np.sqrt(0.75))
    cuts = 3
    per = pts // cuts

    def remote(src, dst, send, recv_sem, device):
        return pltpu.make_async_remote_copy(
            src_ref=src, dst_ref=dst, send_sem=send, recv_sem=recv_sem,
            device_id=device, device_id_type=mesh_id,
        )

    def share(blk, lane, slot, p, target):
        piece = buf.at[blk, slot, pl.ds(per * p, per)]
        return remote(piece, piece, ssem.at[blk, lane, p], rsem.at[blk, slot, p], (band, target))

    def near(blk, p):
        at = pl.ds(per * p, per)
        device = (above if blk == 1 else below, cross)
        return remote(buf.at[0, me, at], buf.at[blk, me, at], nsem.at[blk - 1, p], rsem.at[blk, me, p], device)

    def onward(blk, p):
        at = pl.ds(per * p, per)
        device = (above if blk == 1 else below, cross)
        return remote(buf.at[0, cross, at], buf.at[blk, cross, at], fsem.at[blk - 1], rsem.at[blk, cross, p], device)

    def each(n, body):
        def one(k, _):
            body(k)
            return 0

        lax.fori_loop(0, n, one, 0)

    def lay_own(q):
        for h in range(2):
            for r in range(pts):
                for j in range(width // 128):
                    unit = ((2 * q + h) * pts + r) * (width // 128) + j
                    piece = orb_ref[bands * unit : bands * unit + bands, :]
                    at = (me, r, pl.ds(8 * q + 4 * h, bands), pl.ds(128 * j, 128))
                    buf[(0,) + at] = piece

    for q in range(xs // 2):
        lay_own(q)

    lanes = width // 128
    tile, nall = 8, nband * bands

    def tile_of(c):
        return pl.ds(pl.multiple_of(c // lanes * tile, tile), tile), pl.ds(pl.multiple_of(c % lanes * 128, 128), 128)

    def part_orb(c):
        row, lane = tile_of(c)
        mine = ro.at[pl.ds(band * bands, bands)]
        return remote(ox.at[:, row, lane], mine, so.at[c], qo.at[band], (c, cross))

    def part_vec(slot, c):
        row, lane = tile_of(c)
        return remote(vec.at[slot, row, lane], rv.at[band * bands + me], sv.at[slot], qv, (c, (slot + 2) % 4))

    def send_vec(slot):
        def one(k):
            c = target(k)
            own = jnp.logical_and(c == band, (slot + 2) % 4 == me)

            @pl.when(jnp.logical_not(own))
            def _():
                part_vec(slot, c).start()

            @pl.when(own)
            def _():
                row, lane = tile_of(c)
                rv[band * bands + me] = vec[slot, row, lane]

        each(count, one)

    def lay_orb():
        for r in range(pts):
            for j in range(lanes):
                for b in range(bands):
                    first = bands * (lanes * r + j) + b
                    rows_b = orb_ref[pl.ds(first, xs, stride=pts * lanes * bands), :]
                    ox[b, xs * r : xs * r + xs, 128 * j : 128 * j + 128] = rows_b

    def target(k):
        return (band + k) % count

    def term(b):
        return remote(gs.at[b], gr.at[band], sg.at[b], qg.at[band], (b, cross))

    def take(src):
        flat = src.reshape(nall * tile, 128)
        return split(jnp.concatenate([flat[pl.ds(r, nall, stride=tile), :] for r in range(tile)], axis=1))

    def nt(a, b):
        return lax.dot_general(a, b, (((1,), (1,)), ((), ())), preferred_element_type=jnp.float32)

    def swap(slot):
        return remote(ps, pr.at[me], sp.at[slot], qp.at[me], (band, slot))

    def tiles(n, sem):
        return remote(rv.at[pl.ds(0, n)], rv.at[pl.ds(0, n)], sem, qv, (band, sib))

    barrier = pltpu.get_barrier_semaphore()
    each(nband, lambda b: pl.semaphore_signal(barrier, inc=1, device_id=(b, cross), device_id_type=mesh_id))
    for other in (sib, far):
        pl.semaphore_signal(barrier, inc=1, device_id=(band, other), device_id_type=mesh_id)
    pl.semaphore_wait(barrier, nband + 2)

    for p in range(cuts):
        share(0, 1, me, p, cross).start()
    for p in range(cuts):
        share(0, 0, me, p, sib).start()
    for p in range(cuts):
        near(1, p).start()

    def weights(first, last, cols):
        def one(u, _):
            at = pl.ds(pl.multiple_of(u * ng, 16), ng)
            for d in range(2):
                hi, lo = split(hz_ref[:, :cols] * mix_ref[d, pl.ds(u, 1), :cols])
                wh[d, at, :cols] = hi
                wl[d, at, :cols] = lo
            return 0

        lax.fori_loop(first, last, one, 0)

    weights(0, 2 * step, width)
    weights(2 * step, PTS * step, 2 * width)

    def spread_rows(t):
        upper = lax.broadcasted_iota(jnp.int32, (8, total), 0) < 4
        a = jnp.broadcast_to(kt_ref[pl.ds(2 * t, 1), :], (8, total))
        b = jnp.broadcast_to(kt_ref[pl.ds(2 * t + 1, 1), :], (8, total))
        kx[pl.ds(pl.multiple_of(8 * t, 8), 8), :] = jnp.where(upper, a, b)

    each(ng // 2, spread_rows)
    lay_orb()

    def arrived(blk, slot, p):
        share(blk, 0, slot, p, sib).wait_recv()

    def relay(blk, slot, p):
        arrived(blk, slot, p)
        share(blk, 2, slot, p, sib).start()

    def spread(blk, p, wide):
        arrived(blk, cross, p)
        if wide:
            share(blk, 1, cross, p, cross).start()
        share(blk, 0, cross, p, sib).start()

    def slot_of(blk, s):
        turn = s // 2 + jnp.minimum(blk, 1)
        return ((chip + turn) % 2) * 2 + (core + s % 2) % 2

    def amplitude(slot):
        sub = lax.broadcasted_iota(jnp.int32, (8, 128), 0)
        pick = sub // bands * bands + me

        def one(r):
            for q in range(rows // 8):
                for j in range(width // 128):
                    at = (slot, r, pl.ds(8 * q, 8), pl.ds(128 * j, 128))
                    amp[at] = jnp.take_along_axis(buf[(0,) + at], pick, axis=0)

        each(pts, one)

    def pieces():
        for q in range(rows // 16):
            for j in range(width // 128):
                yield q, j

    def forward(blk, s):
        slot = slot_of(blk, s)

        @pl.when(jnp.logical_and(blk == 0, s == 2))
        def _():
            for p in range(cuts):
                relay(0, cross, p)
                if p == 0:
                    onward(1, 0).start()
                    for k in range(cuts):
                        near(2, k).start()
                if p == cuts - 1:
                    onward(2, p).start()
                spread(1, p, p > 0)

        @pl.when(jnp.logical_and(blk == 1, s == 2))
        def _():
            spread(2, 1, True)

        @pl.when(s % 2 == 1)
        def _():
            for p in range(cuts):
                arrived(blk, slot, p)

        @pl.when(blk == 0)
        def _():
            amplitude(slot)

        for q, j in pieces():
            at = (pl.ds(16 * q, 16), pl.ds(128 * j, 128))
            f = [amp[(slot, r) + at] * buf[(blk, slot, r) + at] for r in range(PTS)]
            sa, sb, sc = f[0] + f[3], f[1] + f[4], f[2] + f[5]
            da, db, dc = f[0] - f[3], f[1] - f[4], f[2] - f[5]
            even, odd = sb + sc, db - dc
            comps = (sa + even, da - odd, da + 0.5 * odd, root * (db + dc), sa - 0.5 * even, root * (sb - sc))
            to = pl.ds(pl.multiple_of(slot * rows + 16 * q, 16), 16)
            for c, v in enumerate(comps):
                hi, lo = split(v)
                ch[to, c * width + 128 * j : c * width + 128 * j + 128] = hi
                cl[to, c * width + 128 * j : c * width + 128 * j + 128] = lo

    groups = ((0, 1), (1, 1), (2, 2), (4, 2))

    def planar(d, ah, al, emit):
        for first, count in groups:
            lo, size = first * width, count * width
            for n in range(0, size, 256):
                w = min(256, size - n)
                a, b = ah[:, lo : lo + size], al[:, lo : lo + size]
                g, h = wh[d, lo : lo + size, n : n + w], wl[d, lo : lo + size, n : n + w]
                emit(lo + n, w, mm(a, g) + mm(b, g) + mm(a, h))

    def keep_split(at, w, v):
        zh[:, at : at + w], zl[:, at : at + w] = split(v)

    def keep(at, w, v):
        cb[:, at : at + w] = v

    def xpass(h, l):
        return mm(xh_ref[...], h) + mm(xh_ref[...], l) + mm(xl_ref[...], h)

    def xconv():
        for n in range(0, total, 256):
            h, l = split(xpass(zh[:, n : n + 256], zl[:, n : n + 256]) * kx[:, n : n + 256])
            zh[:, n : n + 256], zl[:, n : n + 256] = split(xpass(h, l))

    def push(slot):
        return remote(vec.at[slot], recv.at[me], osem.at[slot], orsem.at[me], (band, slot))

    def inverse(blk, s):
        slot = ((chip + 1 - s // 2) % 2) * 2 + (core + s % 2 + s // 2) % 2
        fresh = blk == 0
        for q, j in pieces():
            to = pl.ds(pl.multiple_of(slot * rows + 16 * q, 16), 16)
            c0, c3, c1, s1, c2, s2 = [cb[to, c * width + 128 * j : c * width + 128 * j + 128] for c in range(PTS)]
            ea, eb, oa, ob = c0 - 0.5 * c2, root * s2, c3 - 0.5 * c1, root * s1
            even = (c0 + c2, ea + eb, ea - eb)
            odd = (c3 + c1, ob - oa, oa + ob)
            for r in range(PTS):
                v = even[r % 3] + odd[r % 3] if r < 3 else even[r % 3] - odd[r % 3]
                w = v * buf[blk, slot, r, 16 * q : 16 * q + 16, 128 * j : 128 * j + 128]
                at = (slot, j, pl.ds(rows * r + 16 * q, 16))
                acc[at] = jnp.where(fresh, w, acc[at] + w)

        @pl.when(blk == 2)
        def _():
            for j in range(width // 128):
                t = [acc[slot, j, pl.ds(b, pts * xs, stride=bands), :] for b in range(bands)]
                vec[slot, :, 128 * j : 128 * j + 128] = -((t[0] + t[1]) + (t[2] + t[3]))

            send_vec(slot)

    def margin():
        @pl.when(band < count)
        def _():
            each(nband, lambda b: remote(ox.at[:, pl.ds(0, tile), pl.ds(0, 128)], ro.at[pl.ds(b * bands, bands)],
                                         so.at[0], qo.at[b], (b, cross)).wait_recv())
            xo[...], xv[...] = take(ro)
            tiles(nall - 1, sv.at[0]).wait_recv()
            vh, vl = take(rv)
            g = nt(vh, xo[...]) + nt(vh, xv[...]) + nt(vl, xo[...])
            for b in range(nband):
                gs[b] = g[4 * b : 4 * b + 4]
            each(nband, lambda k: term((band + k) % nband).start())

        collect()

        def gather(c):
            remote(gs.at[0], gr.at[c], sg.at[0], qg.at[c], (c, cross)).wait_recv()

        each(count, gather)
        sums = gr[0]
        for c in range(1, count):
            sums += gr[c]
        ps[...] = sums
        for slot in (cross, far, sib):
            swap(slot).start()
        for slot in (cross, far, sib):
            remote(ps, pr.at[slot], sp.at[slot], qp.at[slot], (band, slot)).wait()
        pr[me] = sums
        full = ((pr[0] + pr[1]) + (pr[2] + pr[3])) * (1.0 / ng**3)
        for k in range(4):
            @pl.when(me == k)
            def _():
                m_ref[...] = full[:, k * m_ref.shape[1] : (k + 1) * m_ref.shape[1]]

    def block(blk):
        each(4, lambda s: forward(blk, s))
        planar(0, ch, cl, keep_split)

        @pl.when(blk == 1)
        def _():
            spread(2, 2, False)

        xconv()
        planar(1, zh, zl, keep)

        @pl.when(blk == 0)
        def _():
            spread(2, 0, True)
            for p in range(cuts):
                relay(1, me, p)

        @pl.when(blk == 1)
        def _():
            for p in range(cuts):
                relay(2, me, p)
            each(count, lambda k: part_orb(target(k)).start())

        each(4, lambda s: inverse(blk, s))

    each(3, block)

    def place(slot, src):
        for r in range(pts):
            for j in range(width // 128):
                piece = src[xs * r : xs * r + xs, 128 * j : 128 * j + 128]
                o_ref[pl.ds(bands * (width // 128 * r + j) + slot, xs, stride=pts * width // 128 * bands), :] = piece

    for slot in (cross, far, sib):
        push(slot).start()

    def collect():
        recv[me] = vec[me]
        for slot in (sib, cross, far):
            remote(vec.at[slot], recv.at[slot], osem.at[slot], orsem.at[slot], (band, slot)).wait()
        for k in range(4):
            place(k, recv[k])

    margin()
    each(count, lambda k: part_orb(k).wait_send())
    for slot in range(4):
        tiles(count - 1, sv.at[slot]).wait_send()

        @pl.when(jnp.logical_or(band >= count, (slot + 2) % 4 != me))
        def _():
            tiles(1, sv.at[slot]).wait_send()

    @pl.when(band < count)
    def _():
        each(nband, lambda k: term(k).wait_send())

    for p in range(cuts):
        for blk in range(3):
            share(blk, 0, me, p, sib).wait_send()
            share(blk, 2, me, p, sib).wait_send()
            if (blk, p) not in ((1, 0), (2, cuts - 1)):
                share(blk, 1, me, p, cross).wait_send()
        near(1, p).wait_send()
        near(2, p).wait_send()
    onward(1, 0).wait_send()
    onward(2, cuts - 1).wait_send()


def solve(orb, bands, groups, nband, ng):
    width = ng * ng // PTS
    pts, rows = PTS, orb.shape[0] * 128 // (PTS * width)
    step = ng // PTS
    total = pts * width
    xh, xl = split_const(np.kron(hartley(ng), np.eye(bands)))
    hz = np.tile(hartley(ng), (1, 2 * step)).astype(np.float32)
    kt = (kernel_values(ng).astype(np.float32) / np.float32(ng**3)).reshape(ng, total)
    consts = [kt, hz, mixer_rows(ng).astype(np.float32), xh, xl]
    full = (groups, pts, rows, width)
    f32, bf16, dma = jnp.float32, jnp.bfloat16, pltpu.SemaphoreType.DMA
    tall = groups * rows
    xs = rows // bands
    count, nall = orb.shape[0] // bands // 8, nband * bands
    vmem = pl.BlockSpec(memory_space=pltpu.VMEM)
    return pl.pallas_call(
        functools.partial(solve_kernel, ng, count),
        out_shape=[jax.ShapeDtypeStruct(orb.shape, f32), jax.ShapeDtypeStruct((bands, nall // groups), f32)],
        in_specs=[vmem] * 6,
        out_specs=[vmem] * 2,
        scratch_shapes=[
            pltpu.VMEM((3,) + full, f32), pltpu.VMEM(full, f32),
            pltpu.VMEM((groups, width // 128, pts * rows, 128), f32),
            pltpu.VMEM((tall, total), bf16), pltpu.VMEM((tall, total), bf16),
            pltpu.VMEM((tall, total), bf16), pltpu.VMEM((tall, total), bf16),
            pltpu.VMEM((tall, total), f32),
            pltpu.VMEM((2, total, 2 * width), bf16), pltpu.VMEM((2, total, 2 * width), bf16),
            pltpu.VMEM((tall, total), f32),
            pltpu.VMEM((groups, pts * xs, width), f32), pltpu.VMEM((groups, pts * xs, width), f32),
            pltpu.VMEM((bands, pts * xs, width), f32),
            pltpu.VMEM((nall, 8, 128), f32), pltpu.VMEM((nall, 8, 128), f32),
            pltpu.VMEM((nall, 1024), bf16), pltpu.VMEM((nall, 1024), bf16),
            pltpu.VMEM((nband, bands, nall), f32), pltpu.VMEM((count, bands, nall), f32),
            pltpu.VMEM((bands, nall), f32), pltpu.VMEM((groups, bands, nall), f32),
            dma((3, groups, 3)), dma((3, 3, 3)), dma((2, 3)), dma((2,)), dma((groups,)), dma((groups,)),
            dma((count,)), dma((groups,)), dma((nband,)), dma(()),
            dma((nband,)), dma((count,)), dma((groups,)), dma((groups,)),
        ],
        compiler_params=pltpu.CompilerParams(
            vmem_limit_bytes=56 * 1024 * 1024, collective_id=0, has_side_effects=True
        ),
        cost_estimate=pl.CostEstimate(flops=10**11, bytes_accessed=10**7, transcendentals=0),
        name="solve",
    )(orb, *[jnp.asarray(c) for c in consts])


def solve(orb, bands, groups, nband, ng):
    width = ng * ng // PTS
    pts, rows = PTS, orb.shape[0] * 128 // (PTS * width)
    step = ng // PTS
    total = pts * width
    xh, xl = split_const(np.kron(hartley(ng), np.eye(bands)))
    hz = np.tile(hartley(ng), (1, 2 * step)).astype(np.float32)
    kt = (kernel_values(ng).astype(np.float32) / np.float32(ng**3)).reshape(ng, total)
    consts = [kt, hz, mixer_rows(ng).astype(np.float32), xh, xl]
    full = (groups, pts, rows, width)
    f32, bf16, dma = jnp.float32, jnp.bfloat16, pltpu.SemaphoreType.DMA
    tall = groups * rows
    xs = rows // bands
    count, nall = orb.shape[0] // bands // 8, nband * bands
    vmem = pl.BlockSpec(memory_space=pltpu.VMEM)
    return pl.pallas_call(
        functools.partial(solve_kernel, ng, count),
        out_shape=[jax.ShapeDtypeStruct(orb.shape, f32), jax.ShapeDtypeStruct((bands, nall // groups), f32)],
        in_specs=[vmem] * 6,
        out_specs=[vmem] * 2,
        scratch_shapes=[
            pltpu.VMEM((3,) + full, f32), pltpu.VMEM(full, f32),
            pltpu.VMEM((groups, width // 128, pts * rows, 128), f32),
            pltpu.VMEM((tall, total), bf16), pltpu.VMEM((tall, total), bf16),
            pltpu.VMEM((tall, total), bf16), pltpu.VMEM((tall, total), bf16),
            pltpu.VMEM((tall, total), f32),
            pltpu.VMEM((2, total, 2 * width), bf16), pltpu.VMEM((2, total, 2 * width), bf16),
            pltpu.VMEM((tall, total), f32),
            pltpu.VMEM((groups, pts * xs, width), f32), pltpu.VMEM((groups, pts * xs, width), f32),
            pltpu.VMEM((bands, pts * xs, width), f32),
            pltpu.VMEM((nall, 8, 128), f32), pltpu.VMEM((nall, 8, 128), f32),
            pltpu.VMEM((nall, 1024), bf16), pltpu.VMEM((nall, 1024), bf16),
            pltpu.VMEM((nband, bands, nall), f32), pltpu.VMEM((count, bands, nall), f32),
            pltpu.VMEM((bands, nall), f32), pltpu.VMEM((groups, bands, nall), f32),
            dma((3, groups, 3)), dma((3, 3, 3)), dma((2, 3)), dma((2,)), dma((groups,)), dma((groups,)),
            dma((count,)), dma((groups,)), dma((nband,)), dma(()),
            dma((nband,)), dma((count,)), dma((groups,)), dma((groups,)),
        ],
        compiler_params=pltpu.CompilerParams(
            vmem_limit_bytes=56 * 1024 * 1024, collective_id=0, has_side_effects=True
        ),
        cost_estimate=pl.CostEstimate(flops=10**11, bytes_accessed=10**7, transcendentals=0),
        name="solve",
    )(orb, *[jnp.asarray(c) for c in consts])


def chunking(local, nband):
    tiles = local // 128
    per = next(p for p in range(1, tiles + 1) if tiles % p == 0 and tiles // p <= nband)
    return tiles // per, per * 128


def on_device(orbitals):
    groups = lax.axis_size("grid")
    bands, local = orbitals.shape
    ncell = local * groups
    ng = round(ncell ** (1 / 3))
    raw = orbitals.reshape(bands, local // 128, 128).transpose(1, 0, 2).reshape(bands * local // 128, 128)
    out, margin = solve(raw, bands, groups, lax.axis_size("band"), ng)
    vectors = out.reshape(local // 128, bands, 128).transpose(1, 0, 2).reshape(bands, local)
    return (vectors, margin.T)


def solution(mesh):
    return jax.shard_map(
        on_device,
        mesh=mesh,
        in_specs=(P("band", "grid"),),
        out_specs=(P("band", "grid"), P("grid", "band")),
        check_vma=False,
    )
```

```python
import functools

import jax
import jax.numpy as jnp
import numpy as np
from jax import lax
from jax.experimental import pallas as pl
from jax.experimental.pallas import tpu as pltpu
from jax.sharding import PartitionSpec as P


PTS = 6


def freq_order(ng):
    step = ng // PTS
    low = np.arange(step) * PTS
    out = [low, low + 3]
    for k in (1, 2):
        out += [low + k, ng - low - k]
    return np.concatenate(out)


def kernel_values(ng):
    freqs = ((np.arange(ng) + ng // 2) % ng - ng // 2).astype(np.float32)
    fy = freqs[freq_order(ng)]
    sq = freqs[:, None, None] ** 2 + fy[None, :, None] ** 2 + freqs[None, None, :] ** 2
    safe = np.where(sq > 0, sq, np.float32(1.0))
    return np.where(sq > 0, 40.0 * (1.0 - np.exp(-sq / 16.0)) / safe, 0.0)


def cas(ang):
    return np.cos(ang) + np.sin(ang)


def hartley(ng):
    k = np.arange(ng)
    return cas((k[:, None] * k[None, :] % ng) * (2.0 * np.pi / ng))


def mixers(ng):
    step = ng // PTS
    s, k2 = np.arange(step)[:, None], np.arange(step)[None, :]
    out = []
    for k1 in (0, 3, 1, 2):
        ang = s * (k1 + PTS * k2) * (2.0 * np.pi / ng)
        p, m = cas(ang), cas(-ang)
        out.append(p if k1 in (0, 3) else np.block([[p, m], [m, -p]]))
    return out


def mixer_rows(ng):
    step = ng // PTS
    fwd, inv = [], []
    for mat in mixers(ng):
        for rows, keep in ((mat, fwd), (mat.T, inv)):
            wide = np.zeros((rows.shape[0], 2 * step))
            wide[:, : rows.shape[1]] = rows
            keep.append(np.repeat(wide, ng, axis=1))
    return np.stack([np.concatenate(fwd), np.concatenate(inv)])


def split_const(table):
    table = np.asarray(table, np.float32)
    hi = table.astype(jnp.bfloat16)
    lo = (table - hi.astype(np.float32)).astype(jnp.bfloat16)
    return hi, lo


def split(v):
    hi = v.astype(jnp.bfloat16)
    lo = (v - hi.astype(jnp.float32)).astype(jnp.bfloat16)
    return hi, lo


def mm(a, b):
    return jnp.dot(a, b, preferred_element_type=jnp.float32)


def solve_kernel(ng, count, orb_ref, kt_ref, hz_ref, mix_ref, xh_ref, xl_ref, o_ref, m_ref,
                 buf, amp, acc, ch, cl, zh, zl, cb, wh, wl, kx, vec, recv,
                 ox, ro, rv, xo, xv, gs, gr,
                 rsem, ssem, nsem, fsem, osem, orsem, so, sv, qo, qv, sg, qg):
    pts, rows, width = buf.shape[2:]
    bands, step = 4, ng // PTS
    xs = rows // bands
    total = pts * width
    me = lax.axis_index("grid")
    band, nband = lax.axis_index("band"), lax.axis_size("band")
    chip, core = me // 2, me % 2
    sib = chip * 2 + (1 - core)
    cross = (1 - chip) * 2 + core
    far = (1 - chip) * 2 + (1 - core)
    above, below = (band + 1) % nband, (band + nband - 1) % nband
    mesh_id = pl.DeviceIdType.MESH
    root = np.float32(np.sqrt(0.75))
    cuts = 3
    per = pts // cuts

    def remote(src, dst, send, recv_sem, device):
        return pltpu.make_async_remote_copy(
            src_ref=src, dst_ref=dst, send_sem=send, recv_sem=recv_sem,
            device_id=device, device_id_type=mesh_id,
        )

    def share(blk, lane, slot, p, target):
        piece = buf.at[blk, slot, pl.ds(per * p, per)]
        return remote(piece, piece, ssem.at[blk, lane, p], rsem.at[blk, slot, p], (band, target))

    def near(blk, p):
        at = pl.ds(per * p, per)
        device = (above if blk == 1 else below, cross)
        return remote(buf.at[0, me, at], buf.at[blk, me, at], nsem.at[blk - 1, p], rsem.at[blk, me, p], device)

    def onward(blk, p):
        at = pl.ds(per * p, per)
        device = (above if blk == 1 else below, cross)
        return remote(buf.at[0, cross, at], buf.at[blk, cross, at], fsem.at[blk - 1], rsem.at[blk, cross, p], device)

    def each(n, body):
        def one(k, _):
            body(k)
            return 0

        lax.fori_loop(0, n, one, 0)

    def lay_own(q):
        for h in range(2):
            for r in range(pts):
                for j in range(width // 128):
                    unit = ((2 * q + h) * pts + r) * (width // 128) + j
                    piece = orb_ref[bands * unit : bands * unit + bands, :]
                    at = (me, r, pl.ds(8 * q + 4 * h, bands), pl.ds(128 * j, 128))
                    buf[(0,) + at] = piece

    for q in range(xs // 2):
        lay_own(q)

    lanes = width // 128
    tile, nall = 8, nband * bands

    deep = pts * xs // tile
    own_row, own_lane = band // lanes, band % lanes
    first_row, first_band = (own_row + deep * 5 // 8) % deep, (band + nband * 5 // 8) % nband

    def wrap(n, top):
        return jnp.where(n >= top, n - top, n)

    def cells(row, j):
        return pl.ds(pl.multiple_of(row * tile, tile), tile), pl.ds(128 * j, 128)

    def part_orb(row, j):
        mine = ro.at[pl.ds(band * bands, bands)]
        r, l = cells(row, j)
        return remote(ox.at[:, r, l], mine, so, qo, (row * lanes + j, cross))

    def send_orb():
        def one(k):
            for j in range(lanes):
                part_orb(wrap(first_row + k, deep), j).start()

        each(deep, one)

    def part_vec(slot, row, j):
        r, l = cells(row, j)
        return remote(vec.at[slot, r, l], rv.at[band * bands + me], sv.at[slot], qv, (row * lanes + j, (slot + 2) % 4))

    def send_vec(slot):
        def one(k):
            row = wrap(first_row + k, deep)
            home = jnp.logical_and(row == own_row, (slot + 2) % 4 == me)

            @pl.when(jnp.logical_not(home))
            def _():
                for j in range(lanes):
                    part_vec(slot, row, j).start()

            @pl.when(home)
            def _():
                for j in range(lanes):
                    @pl.when(own_lane != j)
                    def _():
                        part_vec(slot, row, j).start()

                    @pl.when(own_lane == j)
                    def _():
                        r, l = cells(row, j)
                        rv[band * bands + me] = vec[slot, r, l]

        each(deep, one)

    def lay_orb():
        for r in range(pts):
            for j in range(lanes):
                for b in range(bands):
                    first = bands * (lanes * r + j) + b
                    rows_b = orb_ref[pl.ds(first, xs, stride=pts * lanes * bands), :]
                    ox[b, xs * r : xs * r + xs, 128 * j : 128 * j + 128] = rows_b

    def term(b, g):
        return remote(gs.at[b * bands + g], gr.at[band * bands + me], sg, qg, (b, g))

    def terms(n):
        return remote(gs.at[pl.ds(0, n)], gs.at[pl.ds(0, n)], sg, qg, (band, sib))

    def send_terms():
        def one(k):
            b = wrap(first_band + k, nband)

            @pl.when(b != band)
            def _():
                for g in range(bands):
                    term(b, g).start()

            @pl.when(b == band)
            def _():
                for g in range(bands):
                    @pl.when(me != g)
                    def _():
                        term(b, g).start()

                    @pl.when(me == g)
                    def _():
                        gr[band * bands + me] = gs[b * bands + g]

        each(nband, one)

    def regroup(g):
        sub = lax.broadcasted_iota(jnp.int32, (nall, nall), 0) % bands
        quarter = nall // bands
        lane = lax.broadcasted_iota(jnp.int32, (nall, nall), 1) // quarter
        out = g
        for d in range(1, bands):
            moved = jnp.where(sub >= d, pltpu.roll(g, d, 0), pltpu.roll(g, nall + d - bands, 0))
            moved = pltpu.roll(moved, nall - quarter * d, 1)
            out = jnp.where((sub + bands - lane) % bands == d, moved, out)
        return out

    def take(src):
        flat = src.reshape(nall * tile, 128)
        return split(jnp.concatenate([flat[pl.ds(r, nall, stride=tile), :] for r in range(tile)], axis=1))

    def nt(a, b):
        return lax.dot_general(a, b, (((1,), (1,)), ((), ())), preferred_element_type=jnp.float32)

    def tiles(n, sem):
        return remote(rv.at[pl.ds(0, n)], rv.at[pl.ds(0, n)], sem, qv, (band, sib))

    barrier = pltpu.get_barrier_semaphore()
    each(nband, lambda b: pl.semaphore_signal(barrier, inc=1, device_id=(b, cross), device_id_type=mesh_id))
    for other in (sib, far):
        pl.semaphore_signal(barrier, inc=1, device_id=(band, other), device_id_type=mesh_id)
    pl.semaphore_wait(barrier, nband + 2)

    for p in range(cuts):
        share(0, 1, me, p, cross).start()
    for p in range(cuts):
        share(0, 0, me, p, sib).start()
    for p in range(cuts):
        near(1, p).start()

    def weights(first, last, cols):
        def one(u, _):
            at = pl.ds(pl.multiple_of(u * ng, 16), ng)
            for d in range(2):
                hi, lo = split(hz_ref[:, :cols] * mix_ref[d, pl.ds(u, 1), :cols])
                wh[d, at, :cols] = hi
                wl[d, at, :cols] = lo
            return 0

        lax.fori_loop(first, last, one, 0)

    weights(0, 2 * step, width)
    weights(2 * step, PTS * step, 2 * width)

    def spread_rows(t):
        upper = lax.broadcasted_iota(jnp.int32, (8, total), 0) < 4
        a = jnp.broadcast_to(kt_ref[pl.ds(2 * t, 1), :], (8, total))
        b = jnp.broadcast_to(kt_ref[pl.ds(2 * t + 1, 1), :], (8, total))
        kx[pl.ds(pl.multiple_of(8 * t, 8), 8), :] = jnp.where(upper, a, b)

    each(ng // 2, spread_rows)
    lay_orb()

    def arrived(blk, slot, p):
        share(blk, 0, slot, p, sib).wait_recv()

    def relay(blk, slot, p):
        arrived(blk, slot, p)
        share(blk, 2, slot, p, sib).start()

    def spread(blk, p, wide):
        arrived(blk, cross, p)
        if wide:
            share(blk, 1, cross, p, cross).start()
        share(blk, 0, cross, p, sib).start()

    def slot_of(blk, s):
        turn = s // 2 + jnp.minimum(blk, 1)
        return ((chip + turn) % 2) * 2 + (core + s % 2) % 2

    def amplitude(slot):
        sub = lax.broadcasted_iota(jnp.int32, (8, 128), 0)
        pick = sub // bands * bands + me

        def one(r):
            for q in range(rows // 8):
                for j in range(width // 128):
                    at = (slot, r, pl.ds(8 * q, 8), pl.ds(128 * j, 128))
                    amp[at] = jnp.take_along_axis(buf[(0,) + at], pick, axis=0)

        each(pts, one)

    def pieces():
        for q in range(rows // 16):
            for j in range(width // 128):
                yield q, j

    def forward(blk, s):
        slot = slot_of(blk, s)

        @pl.when(jnp.logical_and(blk == 0, s == 2))
        def _():
            for p in range(cuts):
                relay(0, cross, p)
                if p == 0:
                    onward(1, 0).start()
                    for k in range(cuts):
                        near(2, k).start()
                if p == cuts - 1:
                    onward(2, p).start()
                spread(1, p, p > 0)

        @pl.when(jnp.logical_and(blk == 1, s == 2))
        def _():
            spread(2, 1, True)

        @pl.when(s % 2 == 1)
        def _():
            for p in range(cuts):
                arrived(blk, slot, p)

        @pl.when(blk == 0)
        def _():
            amplitude(slot)

        for q, j in pieces():
            at = (pl.ds(16 * q, 16), pl.ds(128 * j, 128))
            f = [amp[(slot, r) + at] * buf[(blk, slot, r) + at] for r in range(PTS)]
            sa, sb, sc = f[0] + f[3], f[1] + f[4], f[2] + f[5]
            da, db, dc = f[0] - f[3], f[1] - f[4], f[2] - f[5]
            even, odd = sb + sc, db - dc
            comps = (sa + even, da - odd, da + 0.5 * odd, root * (db + dc), sa - 0.5 * even, root * (sb - sc))
            to = pl.ds(pl.multiple_of(slot * rows + 16 * q, 16), 16)
            for c, v in enumerate(comps):
                hi, lo = split(v)
                ch[to, c * width + 128 * j : c * width + 128 * j + 128] = hi
                cl[to, c * width + 128 * j : c * width + 128 * j + 128] = lo

    groups = ((0, 1), (1, 1), (2, 2), (4, 2))

    def planar(d, ah, al, emit, at):
        for first, count in groups:
            lo, size = first * width, count * width
            for n in range(0, size, 256):
                w = min(256, size - n)
                a, b = ah[at, lo : lo + size], al[at, lo : lo + size]
                g, h = wh[d, lo : lo + size, n : n + w], wl[d, lo : lo + size, n : n + w]
                emit(at, slice(lo + n, lo + n + w), mm(a, g) + mm(b, g) + mm(a, h))

    def keep_split(at, to, v):
        zh[at, to], zl[at, to] = split(v)

    def keep(at, to, v):
        cb[at, to] = v

    def xpass(h, l):
        return mm(xh_ref[...], h) + mm(xh_ref[...], l) + mm(xl_ref[...], h)

    def xconv():
        for n in range(0, total, 256):
            h, l = split(xpass(zh[:, n : n + 256], zl[:, n : n + 256]) * kx[:, n : n + 256])
            zh[:, n : n + 256], zl[:, n : n + 256] = split(xpass(h, l))

    def push(slot):
        return remote(vec.at[slot], recv.at[me], osem.at[slot], orsem.at[me], (band, slot))

    def inverse(blk, s):
        slot = ((chip + 1 - s // 2) % 2) * 2 + (core + s % 2 + s // 2) % 2
        fresh = blk == 0
        for q, j in pieces():
            to = pl.ds(pl.multiple_of(slot * rows + 16 * q, 16), 16)
            c0, c3, c1, s1, c2, s2 = [cb[to, c * width + 128 * j : c * width + 128 * j + 128] for c in range(PTS)]
            ea, eb, oa, ob = c0 - 0.5 * c2, root * s2, c3 - 0.5 * c1, root * s1
            even = (c0 + c2, ea + eb, ea - eb)
            odd = (c3 + c1, ob - oa, oa + ob)
            for r in range(PTS):
                v = even[r % 3] + odd[r % 3] if r < 3 else even[r % 3] - odd[r % 3]
                w = v * buf[blk, slot, r, 16 * q : 16 * q + 16, 128 * j : 128 * j + 128]
                at = (slot, j, pl.ds(rows * r + 16 * q, 16))
                acc[at] = jnp.where(fresh, w, acc[at] + w)

        @pl.when(blk == 2)
        def _():
            for j in range(width // 128):
                t = [acc[slot, j, pl.ds(b, pts * xs, stride=bands), :] for b in range(bands)]
                vec[slot, :, 128 * j : 128 * j + 128] = -((t[0] + t[1]) + (t[2] + t[3]))

            send_vec(slot)

    def margin():
        @pl.when(band < count)
        def _():
            remote(ro, ro, so, qo, (band, cross)).wait_recv()
            xo[...], xv[...] = take(ro)
            tiles(nall - 1, sv.at[0]).wait_recv()
            vh, vl = take(rv)
            g = nt(vh, xo[...]) + nt(vh, xv[...]) + nt(vl, xo[...])
            g = regroup(g)
            for n in range(nall):
                gs[n] = g[n : n + 1]
            send_terms()

        collect()
        drain()

        held = count * bands
        @pl.when(band < count)
        def _():
            terms(held - 1).wait_recv()

        @pl.when(band >= count)
        def _():
            terms(held).wait_recv()

        sums = [gr[n] for n in range(4)]
        for n in range(4, held):
            sums[n % 4] += gr[n]
        full = ((sums[0] + sums[1]) + (sums[2] + sums[3])) * (1.0 / ng**3)
        for k in range(bands):
            m_ref[k : k + 1, :] = full[:, k * m_ref.shape[1] : (k + 1) * m_ref.shape[1]]

    def block(blk):
        def half(h):
            forward(blk, 2 * h)
            forward(blk, 2 * h + 1)
            which = (chip + jnp.minimum(blk, 1) + h) % 2
            planar(0, ch, cl, keep_split, pl.ds(pl.multiple_of(which * 2 * rows, 32), 2 * rows))

        each(2, half)

        @pl.when(blk == 1)
        def _():
            spread(2, 2, False)

        xconv()
        planar(1, zh, zl, keep, slice(None))

        @pl.when(blk == 0)
        def _():
            spread(2, 0, True)
            for p in range(cuts):
                relay(1, me, p)

        @pl.when(blk == 1)
        def _():
            for p in range(cuts):
                relay(2, me, p)
            send_orb()

        each(4, lambda s: inverse(blk, s))

    each(3, block)

    def place(slot, src):
        for r in range(pts):
            for j in range(width // 128):
                piece = src[xs * r : xs * r + xs, 128 * j : 128 * j + 128]
                o_ref[pl.ds(bands * (width // 128 * r + j) + slot, xs, stride=pts * width // 128 * bands), :] = piece

    for slot in (cross, far, sib):
        push(slot).start()

    def collect():
        recv[me] = vec[me]
        for slot in (sib, cross, far):
            remote(vec.at[slot], recv.at[slot], osem.at[slot], orsem.at[slot], (band, slot)).wait()
        for k in range(4):
            place(k, recv[k])

    def drain():
        remote(ox, ox, so, qo, (band, cross)).wait_send()
        for slot in range(4):
            home = jnp.logical_and(band < count, (slot + 2) % 4 == me)

            @pl.when(home)
            def _():
                tiles(count - 1, sv.at[slot]).wait_send()

            @pl.when(jnp.logical_not(home))
            def _():
                tiles(count, sv.at[slot]).wait_send()

        for p in range(cuts):
            for blk in range(3):
                share(blk, 0, me, p, sib).wait_send()
                share(blk, 2, me, p, sib).wait_send()
                if (blk, p) not in ((1, 0), (2, cuts - 1)):
                    share(blk, 1, me, p, cross).wait_send()
            near(1, p).wait_send()
            near(2, p).wait_send()
        onward(1, 0).wait_send()
        onward(2, cuts - 1).wait_send()

    margin()

    @pl.when(band < count)
    def _():
        terms(nall - 1).wait_send()


def solve(orb, bands, groups, nband, ng):
    width = ng * ng // PTS
    pts, rows = PTS, orb.shape[0] * 128 // (PTS * width)
    step = ng // PTS
    total = pts * width
    xh, xl = split_const(np.kron(hartley(ng), np.eye(bands)))
    hz = np.tile(hartley(ng), (1, 2 * step)).astype(np.float32)
    kt = (kernel_values(ng).astype(np.float32) / np.float32(ng**3)).reshape(ng, total)
    consts = [kt, hz, mixer_rows(ng).astype(np.float32), xh, xl]
    full = (groups, pts, rows, width)
    f32, bf16, dma = jnp.float32, jnp.bfloat16, pltpu.SemaphoreType.DMA
    tall = groups * rows
    xs = rows // bands
    count, nall = orb.shape[0] // bands // 8, nband * bands
    vmem = pl.BlockSpec(memory_space=pltpu.VMEM)
    return pl.pallas_call(
        functools.partial(solve_kernel, ng, count),
        out_shape=[pltpu.VMEM(orb.shape, f32), pltpu.VMEM((bands, nall // groups), f32)],
        in_specs=[vmem] * 6,
        out_specs=[vmem] * 2,
        scratch_shapes=[
            pltpu.VMEM((3,) + full, f32), pltpu.VMEM(full, f32),
            pltpu.VMEM((groups, width // 128, pts * rows, 128), f32),
            pltpu.VMEM((tall, total), bf16), pltpu.VMEM((tall, total), bf16),
            pltpu.VMEM((tall, total), bf16), pltpu.VMEM((tall, total), bf16),
            pltpu.VMEM((tall, total), f32),
            pltpu.VMEM((2, total, 2 * width), bf16), pltpu.VMEM((2, total, 2 * width), bf16),
            pltpu.VMEM((tall, total), f32),
            pltpu.VMEM((groups, pts * xs, width), f32), pltpu.VMEM((groups, pts * xs, width), f32),
            pltpu.VMEM((bands, pts * xs, width), f32),
            pltpu.VMEM((nall, 8, 128), f32), pltpu.VMEM((nall, 8, 128), f32),
            pltpu.VMEM((nall, 1024), bf16), pltpu.VMEM((nall, 1024), bf16),
            pltpu.VMEM((nall, 1, nall), f32), pltpu.VMEM((count * groups, 1, nall), f32),
            dma((3, groups, 3)), dma((3, 3, 3)), dma((2, 3)), dma((2,)), dma((groups,)), dma((groups,)),
            dma(()), dma((groups,)), dma(()), dma(()),
            dma(()), dma(()),
        ],
        compiler_params=pltpu.CompilerParams(
            vmem_limit_bytes=56 * 1024 * 1024, collective_id=0, has_side_effects=True
        ),
        cost_estimate=pl.CostEstimate(flops=10**11, bytes_accessed=10**7, transcendentals=0),
        name="solve",
    )(orb, *[jnp.asarray(c) for c in consts])


def on_device(orbitals):
    groups = lax.axis_size("grid")
    bands, local = orbitals.shape
    ncell = local * groups
    ng = round(ncell ** (1 / 3))
    raw = orbitals.reshape(bands, local // 128, 128).transpose(1, 0, 2).reshape(bands * local // 128, 128)
    out, margin = solve(raw, bands, groups, lax.axis_size("band"), ng)
    vectors = out.reshape(local // 128, bands, 128).transpose(1, 0, 2).reshape(bands, local)
    return (vectors, margin.T)


def solution(mesh):
    return jax.shard_map(
        on_device,
        mesh=mesh,
        in_specs=(P("band", "grid"),),
        out_specs=(P("band", "grid"), P("grid", "band")),
        check_vma=False,
    )
```

```python
import functools

import jax
import jax.numpy as jnp
import numpy as np
from jax import lax
from jax.experimental import pallas as pl
from jax.experimental.pallas import tpu as pltpu
from jax.sharding import PartitionSpec as P


PTS = 6


def freq_order(ng):
    step = ng // PTS
    low = np.arange(step) * PTS
    out = [low, low + 3]
    for k in (1, 2):
        out += [low + k, ng - low - k]
    return np.concatenate(out)


def kernel_values(ng):
    freqs = ((np.arange(ng) + ng // 2) % ng - ng // 2).astype(np.float32)
    fy = freqs[freq_order(ng)]
    sq = freqs[:, None, None] ** 2 + fy[None, :, None] ** 2 + freqs[None, None, :] ** 2
    safe = np.where(sq > 0, sq, np.float32(1.0))
    return np.where(sq > 0, 40.0 * (1.0 - np.exp(-sq / 16.0)) / safe, 0.0)


def cas(ang):
    return np.cos(ang) + np.sin(ang)


def hartley(ng):
    k = np.arange(ng)
    return cas((k[:, None] * k[None, :] % ng) * (2.0 * np.pi / ng))


def mixers(ng):
    step = ng // PTS
    s, k2 = np.arange(step)[:, None], np.arange(step)[None, :]
    out = []
    for k1 in (0, 3, 1, 2):
        ang = s * (k1 + PTS * k2) * (2.0 * np.pi / ng)
        p, m = cas(ang), cas(-ang)
        out.append(p if k1 in (0, 3) else np.block([[p, m], [m, -p]]))
    return out


def mixer_rows(ng):
    step = ng // PTS
    fwd, inv = [], []
    for mat in mixers(ng):
        for rows, keep in ((mat, fwd), (mat.T, inv)):
            wide = np.zeros((rows.shape[0], 2 * step))
            wide[:, : rows.shape[1]] = rows
            keep.append(np.repeat(wide, ng, axis=1))
    return np.stack([np.concatenate(fwd), np.concatenate(inv)])


def split_const(table):
    table = np.asarray(table, np.float32)
    hi = table.astype(jnp.bfloat16)
    lo = (table - hi.astype(np.float32)).astype(jnp.bfloat16)
    return hi, lo


def split(v):
    hi = v.astype(jnp.bfloat16)
    lo = (v - hi.astype(jnp.float32)).astype(jnp.bfloat16)
    return hi, lo


def mm(a, b):
    return jnp.dot(a, b, preferred_element_type=jnp.float32)


def solve_kernel(ng, orb_ref, kt_ref, hz_ref, mix_ref, xh_ref, xl_ref, o_ref, m_ref,
                 buf, amp, acc, ch, cl, zh, zl, cb, wh, wl, kx, vec, recv,
                 ox, st, ro, rv, xo, xv, ga, gs, gr,
                 rsem, ssem, nsem, fsem, osem, orsem, so, sv, qo, qv, sg, qg):
    pts, rows, width = buf.shape[2:]
    bands, step = 4, ng // PTS
    xs = rows // bands
    total = pts * width
    me = lax.axis_index("grid")
    band, nband = lax.axis_index("band"), lax.axis_size("band")
    chip, core = me // 2, me % 2
    sib = chip * 2 + (1 - core)
    cross = (1 - chip) * 2 + core
    far = (1 - chip) * 2 + (1 - core)
    above, below = (band + 1) % nband, (band + nband - 1) % nband
    mesh_id = pl.DeviceIdType.MESH
    root = np.float32(np.sqrt(0.75))
    cuts = 3
    per = pts // cuts

    def remote(src, dst, send, recv_sem, device):
        return pltpu.make_async_remote_copy(
            src_ref=src, dst_ref=dst, send_sem=send, recv_sem=recv_sem,
            device_id=device, device_id_type=mesh_id,
        )

    def share(blk, lane, slot, p, target):
        piece = buf.at[blk, slot, pl.ds(per * p, per)]
        return remote(piece, piece, ssem.at[blk, lane, p], rsem.at[blk, slot, p], (band, target))

    def near(blk, p):
        at = pl.ds(per * p, per)
        device = (above if blk == 1 else below, cross)
        return remote(buf.at[0, me, at], buf.at[blk, me, at], nsem.at[blk - 1, p], rsem.at[blk, me, p], device)

    def onward(blk, p):
        at = pl.ds(per * p, per)
        device = (above if blk == 1 else below, cross)
        return remote(buf.at[0, cross, at], buf.at[blk, cross, at], fsem.at[blk - 1], rsem.at[blk, cross, p], device)

    def each(n, body):
        def one(k, _):
            body(k)
            return 0

        lax.fori_loop(0, n, one, 0)

    def lay_own(q):
        for h in range(2):
            for r in range(pts):
                for j in range(width // 128):
                    unit = ((2 * q + h) * pts + r) * (width // 128) + j
                    piece = orb_ref[bands * unit : bands * unit + bands, :]
                    at = (me, r, pl.ds(8 * q + 4 * h, bands), pl.ds(128 * j, 128))
                    buf[(0,) + at] = piece

    for q in range(xs // 2):
        lay_own(q)

    lanes = width // 128
    tile, nall = 8, nband * bands
    yy, zz, xh = band % 8 // 2, band // 8, band % 2
    moves = ((0, 0), (1, 0), (3, 0), (0, 1), (0, 3), (1, 1), (1, 3), (2, 0))
    share_of = 2 * len(moves)
    extra = pts * xs * lanes // tile - share_of

    def base(y, z):
        return z % 4 * 8 + y % 4 * 2

    def shade(y, z):
        return (y + z // 2 * 2) % 4 + z % 2 * 4

    targets = [(base(yy + oy, zz + oz), shade((yy + oy) % 4, (zz + oz) % 4)) for oy, oz in moves]
    sources = [base(yy + 4 - oy, zz + 4 - oz) for oy, oz in moves]
    double = shade(yy, zz) + 8 * xh < extra

    def tile_at(t):
        return pl.ds(pl.multiple_of(t * tile, tile), tile)

    def send_orb(src, b):
        mine = pl.ds(b * bands, bands)

        def one(e, y, z, k):
            home = jnp.logical_and(yy == y, zz == z)
            at = tile_at(e + 8 * xh + share_of * k)

            @pl.when(jnp.logical_not(home))
            def _():
                remote(src.at[:, at], ro.at[k, mine], so.at[k], qo.at[k], (base(y, z) + xh, me)).start()

            @pl.when(home)
            def _():
                ro[k, mine] = src[:, at]

        for e in range(8):
            for w in range(2):
                y, z = (e % 4 + 2 * w) % 4, e // 4 + 2 * w
                one(e, y, z, 0)
                if e + 8 < extra:
                    one(e, y, z, 1)
                else:
                    @pl.when(xh == 0)
                    def _():
                        one(e, y, z, 1)

    def orbs(k, n):
        piece = ro.at[k, pl.ds(0, bands * n)]
        return remote(piece, piece, so.at[k], qo.at[k], (band, sib))

    def send_vec(slot):
        def one(i, x, k):
            where, q = targets[i]
            t = q + 8 * x + share_of * k
            index = (i * 2 + xh) * bands + me

            def go():
                remote(vec.at[slot, tile_at(t)], rv.at[k, index], sv.at[k, slot], qv.at[k], (where + x, slot)).start()

            if i > 0:
                go()
                return
            home = jnp.logical_and(xh == x, slot == me)
            pl.when(jnp.logical_not(home))(go)

            @pl.when(home)
            def _():
                rv[k, index] = vec[slot, tile_at(t)]

        for i in range(len(moves) - 1, -1, -1):
            for x in range(2):
                one(i, x, 0)
                if x == 0:
                    one(i, x, 1)
                else:
                    @pl.when(targets[i][1] + 8 < extra)
                    def _():
                        one(i, x, 1)

    def vecs(k, n, slot):
        piece = rv.at[k, pl.ds(0, n)]
        return remote(piece, piece, sv.at[k, slot], qv.at[k], (band, sib))

    def lay_orb():
        for r in range(pts):
            for j in range(lanes):
                for b in range(bands):
                    first = bands * (lanes * r + j) + b
                    rows_b = orb_ref[pl.ds(first, xs, stride=pts * lanes * bands), :]
                    ox[0, b, pts * xs * j + xs * r : pts * xs * j + xs * r + xs, :] = rows_b

    def lay_mate():
        blk = 2 - xh
        for j in range(lanes):
            for r in range(pts):
                st[j, rows * r : rows * r + rows, :] = buf[blk, me, r, :, 128 * j : 128 * j + 128]
            for b in range(bands):
                ox[1, b, pts * xs * j : pts * xs * (j + 1), :] = st[j, pl.ds(b, pts * xs, stride=bands), :]

    def term(m, g):
        return remote(gs.at[m * bands + g], gr.at[(m // 2 * 2 + xh) * bands + me], sg, qg, (sources[m // 2] + m % 2, g))

    def terms(n):
        return remote(gs.at[pl.ds(0, n)], gs.at[pl.ds(0, n)], sg, qg, (band, sib))

    def send_terms():
        for m in range(share_of - 1, -1, -1):
            for g in range(bands):
                if m > 1:
                    term(m, g).start()
                else:
                    home = jnp.logical_and(xh == m, me == g)

                    @pl.when(jnp.logical_not(home))
                    def _():
                        term(m, g).start()

                    @pl.when(home)
                    def _():
                        gr[xh * bands + me] = gs[m * bands + g]

    def regroup(g):
        sub = lax.broadcasted_iota(jnp.int32, g.shape, 0) % bands
        quarter = nall // bands
        lane = lax.broadcasted_iota(jnp.int32, g.shape, 1) // quarter
        out = g
        for d in range(1, bands):
            moved = jnp.where(sub >= d, pltpu.roll(g, d, 0), pltpu.roll(g, g.shape[0] + d - bands, 0))
            moved = pltpu.roll(moved, nall - quarter * d, 1)
            out = jnp.where((sub + bands - lane) % bands == d, moved, out)
        return out

    def take(src, n):
        flat = src.reshape(n * tile, 128)
        return split(jnp.concatenate([flat[pl.ds(r, n, stride=tile), :] for r in range(tile)], axis=1))

    def nt(a, b):
        return lax.dot_general(a, b, (((1,), (1,)), ((), ())), preferred_element_type=jnp.float32)

    barrier = pltpu.get_barrier_semaphore()
    def greet(device):
        pl.semaphore_signal(barrier, inc=1, device_id=device, device_id_type=mesh_id)

    for device in ((band, sib), (band, cross), (band, far), (above, cross), (below, cross)):
        greet(device)
    each(nband - 1, lambda k: greet((jnp.where(k >= band, k + 1, k), me)))
    pl.semaphore_wait(barrier, nband + 4)

    for p in range(cuts):
        share(0, 1, me, p, cross).start()
    for p in range(cuts):
        share(0, 0, me, p, sib).start()
    for p in range(cuts):
        near(1, p).start()

    def weights(first, last, cols):
        def one(u, _):
            at = pl.ds(pl.multiple_of(u * ng, 16), ng)
            for d in range(2):
                hi, lo = split(hz_ref[:, :cols] * mix_ref[d, pl.ds(u, 1), :cols])
                wh[d, at, :cols] = hi
                wl[d, at, :cols] = lo
            return 0

        lax.fori_loop(first, last, one, 0)

    weights(0, 2 * step, width)
    weights(2 * step, PTS * step, 2 * width)

    def spread_rows(t):
        upper = lax.broadcasted_iota(jnp.int32, (8, total), 0) < 4
        a = jnp.broadcast_to(kt_ref[pl.ds(2 * t, 1), :], (8, total))
        b = jnp.broadcast_to(kt_ref[pl.ds(2 * t + 1, 1), :], (8, total))
        kx[pl.ds(pl.multiple_of(8 * t, 8), 8), :] = jnp.where(upper, a, b)

    each(ng // 2, spread_rows)
    lay_orb()

    def arrived(blk, slot, p):
        share(blk, 0, slot, p, sib).wait_recv()

    def relay(blk, slot, p):
        arrived(blk, slot, p)
        share(blk, 2, slot, p, sib).start()

    def spread(blk, p, wide):
        arrived(blk, cross, p)
        if wide:
            share(blk, 1, cross, p, cross).start()
        share(blk, 0, cross, p, sib).start()

    def slot_of(blk, s):
        turn = s // 2 + jnp.minimum(blk, 1)
        return ((chip + turn) % 2) * 2 + (core + s % 2) % 2

    def amplitude(slot):
        sub = lax.broadcasted_iota(jnp.int32, (8, 128), 0)
        pick = sub // bands * bands + me

        def one(r):
            for q in range(rows // 8):
                for j in range(width // 128):
                    at = (slot, r, pl.ds(8 * q, 8), pl.ds(128 * j, 128))
                    amp[at] = jnp.take_along_axis(buf[(0,) + at], pick, axis=0)

        each(pts, one)

    def pieces():
        for q in range(rows // 16):
            for j in range(width // 128):
                yield q, j

    def forward(blk, s):
        slot = slot_of(blk, s)

        @pl.when(jnp.logical_and(blk == 0, s == 2))
        def _():
            for p in range(cuts):
                relay(0, cross, p)
                if p == 0:
                    onward(1, 0).start()
                    for k in range(cuts):
                        near(2, k).start()
                if p == cuts - 1:
                    onward(2, p).start()
                spread(1, p, p > 0)

        @pl.when(jnp.logical_and(blk == 1, s == 2))
        def _():
            spread(2, 1, True)

        @pl.when(s % 2 == 1)
        def _():
            for p in range(cuts):
                arrived(blk, slot, p)

        @pl.when(blk == 0)
        def _():
            amplitude(slot)

        for q, j in pieces():
            at = (pl.ds(16 * q, 16), pl.ds(128 * j, 128))
            f = [amp[(slot, r) + at] * buf[(blk, slot, r) + at] for r in range(PTS)]
            sa, sb, sc = f[0] + f[3], f[1] + f[4], f[2] + f[5]
            da, db, dc = f[0] - f[3], f[1] - f[4], f[2] - f[5]
            even, odd = sb + sc, db - dc
            comps = (sa + even, da - odd, da + 0.5 * odd, root * (db + dc), sa - 0.5 * even, root * (sb - sc))
            to = pl.ds(pl.multiple_of(slot * rows + 16 * q, 16), 16)
            for c, v in enumerate(comps):
                hi, lo = split(v)
                ch[to, c * width + 128 * j : c * width + 128 * j + 128] = hi
                cl[to, c * width + 128 * j : c * width + 128 * j + 128] = lo

    groups = ((0, 1), (1, 1), (2, 2), (4, 2))

    def planar(d, ah, al, emit, at):
        for first, count in groups:
            lo, size = first * width, count * width
            for n in range(0, size, 256):
                w = min(256, size - n)
                a, b = ah[at, lo : lo + size], al[at, lo : lo + size]
                g, h = wh[d, lo : lo + size, n : n + w], wl[d, lo : lo + size, n : n + w]
                emit(at, slice(lo + n, lo + n + w), mm(a, g) + mm(b, g) + mm(a, h))

    def keep_split(at, to, v):
        zh[at, to], zl[at, to] = split(v)

    def keep(at, to, v):
        cb[at, to] = v

    def xpass(h, l):
        return mm(xh_ref[...], h) + mm(xh_ref[...], l) + mm(xl_ref[...], h)

    def xconv():
        for n in range(0, total, 256):
            h, l = split(xpass(zh[:, n : n + 256], zl[:, n : n + 256]) * kx[:, n : n + 256])
            zh[:, n : n + 256], zl[:, n : n + 256] = split(xpass(h, l))

    def push(slot):
        return remote(vec.at[slot], recv.at[me], osem.at[slot], orsem.at[me], (band, slot))

    def inverse(blk, s):
        slot = ((chip + 1 - s // 2) % 2) * 2 + (core + s % 2 + s // 2) % 2
        fresh = blk == 0
        for q, j in pieces():
            to = pl.ds(pl.multiple_of(slot * rows + 16 * q, 16), 16)
            c0, c3, c1, s1, c2, s2 = [cb[to, c * width + 128 * j : c * width + 128 * j + 128] for c in range(PTS)]
            ea, eb, oa, ob = c0 - 0.5 * c2, root * s2, c3 - 0.5 * c1, root * s1
            even = (c0 + c2, ea + eb, ea - eb)
            odd = (c3 + c1, ob - oa, oa + ob)
            for r in range(PTS):
                v = even[r % 3] + odd[r % 3] if r < 3 else even[r % 3] - odd[r % 3]
                w = v * buf[blk, slot, r, 16 * q : 16 * q + 16, 128 * j : 128 * j + 128]
                at = (slot, j, pl.ds(rows * r + 16 * q, 16))
                acc[at] = jnp.where(fresh, w, acc[at] + w)

        @pl.when(blk == 2)
        def _():
            for j in range(width // 128):
                t = [acc[slot, j, pl.ds(b, pts * xs, stride=bands), :] for b in range(bands)]
                vec[slot, pts * xs * j : pts * xs * (j + 1), :] = -((t[0] + t[1]) + (t[2] + t[3]))

            send_vec(slot)

    def product(k):
        vh, vl = take(rv.at[k], share_of * bands)
        return nt(vh, xo[k]) + nt(vh, xv[k]) + nt(vl, xo[k])

    def margin():
        others = 2 * (nband // 2 - 1)
        orbs(0, others).wait_recv()
        xo[0], xv[0] = take(ro.at[0], nall)

        @pl.when(double)
        def _():
            orbs(1, others).wait_recv()
            xo[1], xv[1] = take(ro.at[1], nall)

        vecs(0, share_of * bands - 1, 0).wait_recv()
        ga[...] = product(0)

        @pl.when(double)
        def _():
            vecs(1, share_of * bands - 1, 0).wait_recv()
            ga[...] += product(1)

        g = regroup(ga[...])
        for n in range(share_of * bands):
            gs[n] = g[n : n + 1]
        send_terms()
        collect()
        drain()
        held = share_of * bands
        terms(held - 1).wait_recv()
        sums = [gr[n] for n in range(4)]
        for n in range(4, held):
            sums[n % 4] += gr[n]
        full = ((sums[0] + sums[1]) + (sums[2] + sums[3])) * (1.0 / ng**3)
        for k in range(bands):
            m_ref[k : k + 1, :] = full[:, k * m_ref.shape[1] : (k + 1) * m_ref.shape[1]]

    def block(blk):
        def half(h):
            forward(blk, 2 * h)
            forward(blk, 2 * h + 1)
            which = (chip + jnp.minimum(blk, 1) + h) % 2
            planar(0, ch, cl, keep_split, pl.ds(pl.multiple_of(which * 2 * rows, 32), 2 * rows))

        @pl.when(blk < 2)
        def _():
            each(2, half)

        @pl.when(blk == 2)
        def _():
            each(4, lambda s: forward(blk, s))
            planar(0, ch, cl, keep_split, slice(None))


        xconv()

        @pl.when(blk == 1)
        def _():
            spread(2, 2, False)
            send_orb(ox.at[0], band)

        planar(1, zh, zl, keep, slice(None))

        @pl.when(blk == 0)
        def _():
            spread(2, 0, True)
            for p in range(cuts):
                relay(1, me, p)

        @pl.when(blk == 1)
        def _():
            for p in range(cuts):
                relay(2, me, p)
            lay_mate()
            send_orb(ox.at[1], band + 1 - 2 * xh)

        each(4, lambda s: inverse(blk, s))

    each(3, block)

    def place(slot, src):
        for r in range(pts):
            for j in range(width // 128):
                piece = src[pts * xs * j + xs * r : pts * xs * j + xs * r + xs, :]
                o_ref[pl.ds(bands * (width // 128 * r + j) + slot, xs, stride=pts * width // 128 * bands), :] = piece

    for slot in (cross, far, sib):
        push(slot).start()

    def collect():
        recv[me] = vec[me]
        for slot in (sib, cross, far):
            remote(vec.at[slot], recv.at[slot], osem.at[slot], orsem.at[slot], (band, slot)).wait()
        for k in range(4):
            place(k, recv[k])

    def drain():
        orbs(0, 2 * (nband // 2 - 1)).wait_send()
        few = 4 * (extra - 8)

        @pl.when(xh == 0)
        def _():
            orbs(1, 2 * (nband // 2 - 1)).wait_send()

        @pl.when(jnp.logical_and(xh == 1, double))
        def _():
            orbs(1, few - 2).wait_send()

        @pl.when(jnp.logical_and(xh == 1, jnp.logical_not(double)))
        def _():
            orbs(1, few).wait_send()

        for slot in range(4):
            @pl.when(me == slot)
            def _():
                vecs(0, share_of - 1, slot).wait_send()

            @pl.when(me != slot)
            def _():
                vecs(0, share_of, slot).wait_send()

            home = jnp.logical_and(double, me == slot)

            @pl.when(home)
            def _():
                vecs(1, extra - 1, slot).wait_send()

            @pl.when(jnp.logical_not(home))
            def _():
                vecs(1, extra, slot).wait_send()

        for p in range(cuts):
            for blk in range(3):
                share(blk, 0, me, p, sib).wait_send()
                share(blk, 2, me, p, sib).wait_send()
                if (blk, p) not in ((1, 0), (2, cuts - 1)):
                    share(blk, 1, me, p, cross).wait_send()
            near(1, p).wait_send()
            near(2, p).wait_send()
        onward(1, 0).wait_send()
        onward(2, cuts - 1).wait_send()

    margin()

    terms(share_of * bands - 1).wait_send()


def solve(orb, bands, groups, nband, ng):
    width = ng * ng // PTS
    pts, rows = PTS, orb.shape[0] * 128 // (PTS * width)
    step = ng // PTS
    total = pts * width
    xh, xl = split_const(np.kron(hartley(ng), np.eye(bands)))
    hz = np.tile(hartley(ng), (1, 2 * step)).astype(np.float32)
    kt = (kernel_values(ng).astype(np.float32) / np.float32(ng**3)).reshape(ng, total)
    consts = [kt, hz, mixer_rows(ng).astype(np.float32), xh, xl]
    full = (groups, pts, rows, width)
    f32, bf16, dma = jnp.float32, jnp.bfloat16, pltpu.SemaphoreType.DMA
    tall = groups * rows
    xs = rows // bands
    nall, flat = nband * bands, orb.shape[0] // bands
    vmem = pl.BlockSpec(memory_space=pltpu.VMEM)
    return pl.pallas_call(
        functools.partial(solve_kernel, ng),
        out_shape=[pltpu.VMEM(orb.shape, f32), pltpu.VMEM((bands, nall // groups), f32)],
        in_specs=[vmem] * 6,
        out_specs=[vmem] * 2,
        scratch_shapes=[
            pltpu.VMEM((3,) + full, f32), pltpu.VMEM(full, f32),
            pltpu.VMEM((groups, width // 128, pts * rows, 128), f32),
            pltpu.VMEM((tall, total), bf16), pltpu.VMEM((tall, total), bf16),
            pltpu.VMEM((tall, total), bf16), pltpu.VMEM((tall, total), bf16),
            pltpu.VMEM((tall, total), f32),
            pltpu.VMEM((2, total, 2 * width), bf16), pltpu.VMEM((2, total, 2 * width), bf16),
            pltpu.VMEM((tall, total), f32),
            pltpu.VMEM((groups, flat, 128), f32), pltpu.VMEM((groups, flat, 128), f32),
            pltpu.VMEM((2, bands, flat, 128), f32), pltpu.VMEM((width // 128, pts * rows, 128), f32),
            pltpu.VMEM((2, nall, 8, 128), f32), pltpu.VMEM((2, nall // 2, 8, 128), f32),
            pltpu.VMEM((2, nall, 1024), bf16), pltpu.VMEM((2, nall, 1024), bf16),
            pltpu.VMEM((nall // 2, nall), f32),
            pltpu.VMEM((nall // 2, 1, nall), f32), pltpu.VMEM((nall // 2, 1, nall), f32),
            dma((3, groups, 3)), dma((3, 3, 3)), dma((2, 3)), dma((2,)), dma((groups,)), dma((groups,)),
            dma((2,)), dma((2, groups)), dma((2,)), dma((2,)),
            dma(()), dma(()),
        ],
        compiler_params=pltpu.CompilerParams(
            vmem_limit_bytes=56 * 1024 * 1024, collective_id=0, has_side_effects=True
        ),
        cost_estimate=pl.CostEstimate(flops=10**11, bytes_accessed=10**7, transcendentals=0),
        name="solve",
    )(orb, *[jnp.asarray(c) for c in consts])


def on_device(orbitals):
    groups = lax.axis_size("grid")
    bands, local = orbitals.shape
    ncell = local * groups
    ng = round(ncell ** (1 / 3))
    raw = orbitals.reshape(bands, local // 128, 128).transpose(1, 0, 2).reshape(bands * local // 128, 128)
    out, margin = solve(raw, bands, groups, lax.axis_size("band"), ng)
    vectors = out.reshape(local // 128, bands, 128).transpose(1, 0, 2).reshape(bands, local)
    return (vectors, margin.T)


def solution(mesh):
    return jax.shard_map(
        on_device,
        mesh=mesh,
        in_specs=(P("band", "grid"),),
        out_specs=(P("band", "grid"), P("grid", "band")),
        check_vma=False,
    )
```

```python
import functools

import jax
import jax.numpy as jnp
import numpy as np
from jax import lax
from jax.experimental import pallas as pl
from jax.experimental.pallas import tpu as pltpu
from jax.sharding import PartitionSpec as P


PTS = 6


def freq_order(ng):
    step = ng // PTS
    low = np.arange(step) * PTS
    out = [low, low + 3]
    for k in (1, 2):
        out += [low + k, ng - low - k]
    return np.concatenate(out)


def kernel_values(ng):
    freqs = ((np.arange(ng) + ng // 2) % ng - ng // 2).astype(np.float32)
    fy = freqs[freq_order(ng)]
    sq = freqs[:, None, None] ** 2 + fy[None, :, None] ** 2 + freqs[None, None, :] ** 2
    safe = np.where(sq > 0, sq, np.float32(1.0))
    return np.where(sq > 0, 40.0 * (1.0 - np.exp(-sq / 16.0)) / safe, 0.0)


def cas(ang):
    return np.cos(ang) + np.sin(ang)


def hartley(ng):
    k = np.arange(ng)
    return cas((k[:, None] * k[None, :] % ng) * (2.0 * np.pi / ng))


def mixers(ng):
    step = ng // PTS
    s, k2 = np.arange(step)[:, None], np.arange(step)[None, :]
    out = []
    for k1 in (0, 3, 1, 2):
        ang = s * (k1 + PTS * k2) * (2.0 * np.pi / ng)
        p, m = cas(ang), cas(-ang)
        out.append(p if k1 in (0, 3) else np.block([[p, m], [m, -p]]))
    return out


def mixer_rows(ng):
    step = ng // PTS
    fwd, inv = [], []
    for mat in mixers(ng):
        for rows, keep in ((mat, fwd), (mat.T, inv)):
            wide = np.zeros((rows.shape[0], 2 * step))
            wide[:, : rows.shape[1]] = rows
            keep.append(np.repeat(wide, ng, axis=1))
    return np.stack([np.concatenate(fwd), np.concatenate(inv)])


def split_const(table):
    table = np.asarray(table, np.float32)
    hi = table.astype(jnp.bfloat16)
    lo = (table - hi.astype(np.float32)).astype(jnp.bfloat16)
    return hi, lo


def split(v):
    hi = v.astype(jnp.bfloat16)
    lo = (v - hi.astype(jnp.float32)).astype(jnp.bfloat16)
    return hi, lo


def mm(a, b):
    return jnp.dot(a, b, preferred_element_type=jnp.float32)


def solve_kernel(ng, orb_in, kt_in, hz_in, mix_in, xh_in, xl_in, o_ref, m_ref,
                 orb_ref, kt_ref, hz_ref, mix_ref, xh_ref, xl_ref,
                 buf, amp, acc, ch, cl, zh, zl, cb, wh, wl, kx, vec, recv,
                 ox, st, ro, rv, xo, xv, ga, gs, gr,
                 rsem, ssem, nsem, fsem, osem, orsem, so, sv, qo, qv, sg, qg, ls):
    pts, rows, width = buf.shape[2:]
    bands, step = 4, ng // PTS
    xs = rows // bands
    total = pts * width
    me = lax.axis_index("grid")
    band, nband = lax.axis_index("band"), lax.axis_size("band")
    chip, core = me // 2, me % 2
    sib = chip * 2 + (1 - core)
    cross = (1 - chip) * 2 + core
    far = (1 - chip) * 2 + (1 - core)
    above, below = (band + 1) % nband, (band + nband - 1) % nband
    mesh_id = pl.DeviceIdType.MESH
    root = np.float32(np.sqrt(0.75))
    cuts = 3
    per = pts // cuts

    def remote(src, dst, send, recv_sem, device):
        return pltpu.make_async_remote_copy(
            src_ref=src, dst_ref=dst, send_sem=send, recv_sem=recv_sem,
            device_id=device, device_id_type=mesh_id,
        )

    def share(blk, lane, slot, p, target):
        piece = buf.at[blk, slot, pl.ds(per * p, per)]
        return remote(piece, piece, ssem.at[blk, lane, p], rsem.at[blk, slot, p], (band, target))

    def near(blk, p):
        at = pl.ds(per * p, per)
        device = (above if blk == 1 else below, cross)
        return remote(buf.at[0, me, at], buf.at[blk, me, at], nsem.at[blk - 1, p], rsem.at[blk, me, p], device)

    def onward(blk, p):
        at = pl.ds(per * p, per)
        device = (above if blk == 1 else below, cross)
        return remote(buf.at[0, cross, at], buf.at[blk, cross, at], fsem.at[blk - 1], rsem.at[blk, cross, p], device)

    def each(n, body):
        def one(k, _):
            body(k)
            return 0

        lax.fori_loop(0, n, one, 0)


    lanes = width // 128
    tile, nall = 8, nband * bands
    yy, zz, xh = band % 8 // 2, band // 8, band % 2
    moves = ((0, 0), (1, 0), (3, 0), (0, 1), (0, 3), (1, 1), (1, 3), (2, 0))
    share_of = 2 * len(moves)
    extra = pts * xs * lanes // tile - share_of

    def base(y, z):
        return z % 4 * 8 + y % 4 * 2

    def shade(y, z):
        return (y + z // 2 * 2) % 4 + z % 2 * 4

    targets = [(base(yy + oy, zz + oz), shade((yy + oy) % 4, (zz + oz) % 4)) for oy, oz in moves]
    sources = [base(yy + 4 - oy, zz + 4 - oz) for oy, oz in moves]
    double = shade(yy, zz) + 8 * xh < extra

    def tile_at(t):
        return pl.ds(pl.multiple_of(t * tile, tile), tile)

    def send_orb(src, b):
        mine = pl.ds(b * bands, bands)

        def one(e, y, z, k):
            home = jnp.logical_and(yy == y, zz == z)
            at = tile_at(e + 8 * xh + share_of * k)

            @pl.when(jnp.logical_not(home))
            def _():
                remote(src.at[:, at], ro.at[k, mine], so.at[k], qo.at[k], (base(y, z) + xh, me)).start()

            @pl.when(home)
            def _():
                ro[k, mine] = src[:, at]

        for e in range(8):
            for w in range(2):
                y, z = (e % 4 + 2 * w) % 4, e // 4 + 2 * w
                one(e, y, z, 0)
                if e + 8 < extra:
                    one(e, y, z, 1)
                else:
                    @pl.when(xh == 0)
                    def _():
                        one(e, y, z, 1)

    def orbs(k, n):
        piece = ro.at[k, pl.ds(0, bands * n)]
        return remote(piece, piece, so.at[k], qo.at[k], (band, sib))

    def send_vec(slot):
        def one(i, x, k):
            where, q = targets[i]
            t = q + 8 * x + share_of * k
            index = (i * 2 + xh) * bands + me

            def go():
                remote(vec.at[slot, tile_at(t)], rv.at[k, index], sv.at[k, slot], qv.at[k], (where + x, slot)).start()

            if i > 0:
                go()
                return
            home = jnp.logical_and(xh == x, slot == me)
            pl.when(jnp.logical_not(home))(go)

            @pl.when(home)
            def _():
                rv[k, index] = vec[slot, tile_at(t)]

        for i in range(len(moves) - 1, -1, -1):
            for x in range(2):
                one(i, x, 0)
                if x == 0:
                    one(i, x, 1)
                else:
                    @pl.when(targets[i][1] + 8 < extra)
                    def _():
                        one(i, x, 1)

    def vecs(k, n, slot):
        piece = rv.at[k, pl.ds(0, n)]
        return remote(piece, piece, sv.at[k, slot], qv.at[k], (band, sib))

    def lay_orb():
        for r in range(pts):
            for j in range(lanes):
                for b in range(bands):
                    first = bands * (lanes * r + j) + b
                    rows_b = orb_ref[pl.ds(first, xs, stride=pts * lanes * bands), :]
                    ox[0, b, pts * xs * j + xs * r : pts * xs * j + xs * r + xs, :] = rows_b

    def lay_mate():
        blk = 2 - xh
        for j in range(lanes):
            for r in range(pts):
                st[j, rows * r : rows * r + rows, :] = buf[blk, me, r, :, 128 * j : 128 * j + 128]
            for b in range(bands):
                ox[1, b, pts * xs * j : pts * xs * (j + 1), :] = st[j, pl.ds(b, pts * xs, stride=bands), :]

    def term(m, g):
        return remote(gs.at[m * bands + g], gr.at[(m // 2 * 2 + xh) * bands + me], sg, qg, (sources[m // 2] + m % 2, g))

    def terms(n):
        return remote(gs.at[pl.ds(0, n)], gs.at[pl.ds(0, n)], sg, qg, (band, sib))

    def send_terms():
        for m in range(share_of - 1, -1, -1):
            for g in range(bands):
                if m > 1:
                    term(m, g).start()
                else:
                    home = jnp.logical_and(xh == m, me == g)

                    @pl.when(jnp.logical_not(home))
                    def _():
                        term(m, g).start()

                    @pl.when(home)
                    def _():
                        gr[xh * bands + me] = gs[m * bands + g]

    def regroup(g):
        sub = lax.broadcasted_iota(jnp.int32, g.shape, 0) % bands
        quarter = nall // bands
        lane = lax.broadcasted_iota(jnp.int32, g.shape, 1) // quarter
        out = g
        for d in range(1, bands):
            moved = jnp.where(sub >= d, pltpu.roll(g, d, 0), pltpu.roll(g, g.shape[0] + d - bands, 0))
            moved = pltpu.roll(moved, nall - quarter * d, 1)
            out = jnp.where((sub + bands - lane) % bands == d, moved, out)
        return out

    def take(src, n):
        flat = src.reshape(n * tile, 128)
        return split(jnp.concatenate([flat[pl.ds(r, n, stride=tile), :] for r in range(tile)], axis=1))

    def nt(a, b):
        return lax.dot_general(a, b, (((1,), (1,)), ((), ())), preferred_element_type=jnp.float32)

    barrier = pltpu.get_barrier_semaphore()
    def greet(device):
        pl.semaphore_signal(barrier, inc=1, device_id=device, device_id_type=mesh_id)

    for device in ((band, sib), (band, cross), (band, far), (above, cross), (below, cross)):
        greet(device)
    each(nband - 1, lambda k: greet((jnp.where(k >= band, k + 1, k), me)))
    pairs = ((orb_in, orb_ref), (hz_in, hz_ref), (mix_in, mix_ref), (kt_in, kt_ref), (xh_in, xh_ref), (xl_in, xl_ref))
    loads = [pltpu.make_async_copy(src, dst, ls.at[n]) for n, (src, dst) in enumerate(pairs)]
    for load in loads:
        load.start()
    loads[0].wait()

    def lay_own(q):
        for h in range(2):
            for r in range(pts):
                for j in range(width // 128):
                    unit = ((2 * q + h) * pts + r) * (width // 128) + j
                    piece = orb_ref[bands * unit : bands * unit + bands, :]
                    at = (me, r, pl.ds(8 * q + 4 * h, bands), pl.ds(128 * j, 128))
                    buf[(0,) + at] = piece

    for q in range(xs // 2):
        lay_own(q)
    pl.semaphore_wait(barrier, nband + 4)

    for p in range(cuts):
        share(0, 1, me, p, cross).start()
    for p in range(cuts):
        share(0, 0, me, p, sib).start()
    for p in range(cuts):
        near(1, p).start()

    def weights(first, last, cols):
        def one(u, _):
            at = pl.ds(pl.multiple_of(u * ng, 16), ng)
            for d in range(2):
                hi, lo = split(hz_ref[:, :cols] * mix_ref[d, pl.ds(u, 1), :cols])
                wh[d, at, :cols] = hi
                wl[d, at, :cols] = lo
            return 0

        lax.fori_loop(first, last, one, 0)

    for load in loads[1:]:
        load.wait()
    weights(0, 2 * step, width)
    weights(2 * step, PTS * step, 2 * width)

    def spread_rows(t):
        upper = lax.broadcasted_iota(jnp.int32, (8, total), 0) < 4
        a = jnp.broadcast_to(kt_ref[pl.ds(2 * t, 1), :], (8, total))
        b = jnp.broadcast_to(kt_ref[pl.ds(2 * t + 1, 1), :], (8, total))
        kx[pl.ds(pl.multiple_of(8 * t, 8), 8), :] = jnp.where(upper, a, b)

    each(ng // 2, spread_rows)
    lay_orb()

    def arrived(blk, slot, p):
        share(blk, 0, slot, p, sib).wait_recv()

    def relay(blk, slot, p):
        arrived(blk, slot, p)
        share(blk, 2, slot, p, sib).start()

    def spread(blk, p, wide):
        arrived(blk, cross, p)
        if wide:
            share(blk, 1, cross, p, cross).start()
        share(blk, 0, cross, p, sib).start()

    def slot_of(blk, s):
        turn = s // 2 + jnp.minimum(blk, 1)
        return ((chip + turn) % 2) * 2 + (core + s % 2) % 2

    def amplitude(slot):
        sub = lax.broadcasted_iota(jnp.int32, (8, 128), 0)
        pick = sub // bands * bands + me

        def one(r):
            for q in range(rows // 8):
                for j in range(width // 128):
                    at = (slot, r, pl.ds(8 * q, 8), pl.ds(128 * j, 128))
                    amp[at] = jnp.take_along_axis(buf[(0,) + at], pick, axis=0)

        each(pts, one)

    def pieces():
        for q in range(rows // 16):
            for j in range(width // 128):
                yield q, j

    def forward(blk, s):
        slot = slot_of(blk, s)

        @pl.when(jnp.logical_and(blk == 0, s == 2))
        def _():
            for p in range(cuts):
                relay(0, cross, p)
                if p == 0:
                    near(2, 0).start()
                    onward(1, 0).start()
                    for k in range(1, cuts):
                        near(2, k).start()
                if p == cuts - 1:
                    onward(2, p).start()
                spread(1, p, p > 0)

        @pl.when(s % 2 == 1)
        def _():
            for p in range(cuts):
                arrived(blk, slot, p)

        @pl.when(blk == 0)
        def _():
            amplitude(slot)

        for q, j in pieces():
            at = (pl.ds(16 * q, 16), pl.ds(128 * j, 128))
            f = [amp[(slot, r) + at] * buf[(blk, slot, r) + at] for r in range(PTS)]
            sa, sb, sc = f[0] + f[3], f[1] + f[4], f[2] + f[5]
            da, db, dc = f[0] - f[3], f[1] - f[4], f[2] - f[5]
            even, odd = sb + sc, db - dc
            comps = (sa + even, da - odd, da + 0.5 * odd, root * (db + dc), sa - 0.5 * even, root * (sb - sc))
            to = pl.ds(pl.multiple_of(slot * rows + 16 * q, 16), 16)
            for c, v in enumerate(comps):
                hi, lo = split(v)
                ch[to, c * width + 128 * j : c * width + 128 * j + 128] = hi
                cl[to, c * width + 128 * j : c * width + 128 * j + 128] = lo

    groups = ((0, 1), (1, 1), (2, 2), (4, 2))

    def planar(d, ah, al, emit, at):
        for first, count in groups:
            lo, size = first * width, count * width
            for n in range(0, size, 256):
                w = min(256, size - n)
                a, b = ah[at, lo : lo + size], al[at, lo : lo + size]
                g, h = wh[d, lo : lo + size, n : n + w], wl[d, lo : lo + size, n : n + w]
                emit(at, slice(lo + n, lo + n + w), mm(a, g) + mm(b, g) + mm(a, h))

    def keep_split(at, to, v):
        zh[at, to], zl[at, to] = split(v)

    def keep(at, to, v):
        cb[at, to] = v

    def xpass(h, l):
        return mm(xh_ref[...], h) + mm(xh_ref[...], l) + mm(xl_ref[...], h)

    def xconv():
        for n in range(0, total, 256):
            h, l = split(xpass(zh[:, n : n + 256], zl[:, n : n + 256]) * kx[:, n : n + 256])
            zh[:, n : n + 256], zl[:, n : n + 256] = split(xpass(h, l))

    def push(slot):
        return remote(vec.at[slot], recv.at[me], osem.at[slot], orsem.at[me], (band, slot))

    def inverse(blk, s):
        slot = ((chip + 1 - s // 2) % 2) * 2 + (core + s % 2 + s // 2) % 2
        fresh = blk == 0
        for q, j in pieces():
            to = pl.ds(pl.multiple_of(slot * rows + 16 * q, 16), 16)
            c0, c3, c1, s1, c2, s2 = [cb[to, c * width + 128 * j : c * width + 128 * j + 128] for c in range(PTS)]
            ea, eb, oa, ob = c0 - 0.5 * c2, root * s2, c3 - 0.5 * c1, root * s1
            even = (c0 + c2, ea + eb, ea - eb)
            odd = (c3 + c1, ob - oa, oa + ob)
            for r in range(PTS):
                v = even[r % 3] + odd[r % 3] if r < 3 else even[r % 3] - odd[r % 3]
                w = v * buf[blk, slot, r, 16 * q : 16 * q + 16, 128 * j : 128 * j + 128]
                at = (slot, j, pl.ds(rows * r + 16 * q, 16))
                acc[at] = jnp.where(fresh, w, acc[at] + w)

        @pl.when(blk == 2)
        def _():
            for j in range(width // 128):
                t = [acc[slot, j, pl.ds(b, pts * xs, stride=bands), :] for b in range(bands)]
                vec[slot, pts * xs * j : pts * xs * (j + 1), :] = -((t[0] + t[1]) + (t[2] + t[3]))

            send_vec(slot)

    def product(k):
        vh, vl = take(rv.at[k], share_of * bands)
        return nt(vh, xo[k]) + nt(vh, xv[k]) + nt(vl, xo[k])

    def margin():
        others = 2 * (nband // 2 - 1)
        orbs(0, others).wait_recv()
        xo[0], xv[0] = take(ro.at[0], nall)

        @pl.when(double)
        def _():
            orbs(1, others).wait_recv()
            xo[1], xv[1] = take(ro.at[1], nall)

        vecs(0, share_of * bands - 1, 0).wait_recv()
        ga[...] = product(0)

        @pl.when(double)
        def _():
            vecs(1, share_of * bands - 1, 0).wait_recv()
            ga[...] += product(1)

        g = regroup(ga[...])
        for n in range(share_of * bands):
            gs[n] = g[n : n + 1]
        send_terms()
        collect()
        drain()
        held = share_of * bands
        terms(held - 1).wait_recv()
        sums = [gr[n] for n in range(4)]
        for n in range(4, held):
            sums[n % 4] += gr[n]
        full = ((sums[0] + sums[1]) + (sums[2] + sums[3])) * (1.0 / ng**3)
        for k in range(bands):
            m_ref[k : k + 1, :] = full[:, k * m_ref.shape[1] : (k + 1) * m_ref.shape[1]]

    def block(blk):
        def half(h):
            forward(blk, 2 * h)
            forward(blk, 2 * h + 1)
            which = (chip + jnp.minimum(blk, 1) + h) % 2
            planar(0, ch, cl, keep_split, pl.ds(pl.multiple_of(which * 2 * rows, 32), 2 * rows))

        @pl.when(blk < 2)
        def _():
            each(2, half)

        @pl.when(blk == 2)
        def _():
            each(4, lambda s: forward(blk, s))
            planar(0, ch, cl, keep_split, slice(None))


        @pl.when(blk == 1)
        def _():
            spread(2, 1, True)

        xconv()

        @pl.when(blk == 0)
        def _():
            spread(2, 0, True)

        @pl.when(blk == 1)
        def _():
            spread(2, 2, False)
            send_orb(ox.at[0], band)

        planar(1, zh, zl, keep, slice(None))

        @pl.when(blk == 0)
        def _():
            for p in range(cuts):
                relay(1, me, p)

        @pl.when(blk == 1)
        def _():
            for p in range(cuts):
                relay(2, me, p)
            lay_mate()
            send_orb(ox.at[1], band + 1 - 2 * xh)

        each(4, lambda s: inverse(blk, s))

    each(3, block)

    def place(slot, src):
        for r in range(pts):
            for j in range(width // 128):
                piece = src[pts * xs * j + xs * r : pts * xs * j + xs * r + xs, :]
                o_ref[pl.ds(bands * (width // 128 * r + j) + slot, xs, stride=pts * width // 128 * bands), :] = piece

    for slot in (cross, far, sib):
        push(slot).start()

    def collect():
        recv[me] = vec[me]
        for slot in (sib, cross, far):
            remote(vec.at[slot], recv.at[slot], osem.at[slot], orsem.at[slot], (band, slot)).wait()
        for k in range(4):
            place(k, recv[k])

    def drain():
        orbs(0, 2 * (nband // 2 - 1)).wait_send()
        few = 4 * (extra - 8)

        @pl.when(xh == 0)
        def _():
            orbs(1, 2 * (nband // 2 - 1)).wait_send()

        @pl.when(jnp.logical_and(xh == 1, double))
        def _():
            orbs(1, few - 2).wait_send()

        @pl.when(jnp.logical_and(xh == 1, jnp.logical_not(double)))
        def _():
            orbs(1, few).wait_send()

        for slot in range(4):
            @pl.when(me == slot)
            def _():
                vecs(0, share_of - 1, slot).wait_send()

            @pl.when(me != slot)
            def _():
                vecs(0, share_of, slot).wait_send()

            home = jnp.logical_and(double, me == slot)

            @pl.when(home)
            def _():
                vecs(1, extra - 1, slot).wait_send()

            @pl.when(jnp.logical_not(home))
            def _():
                vecs(1, extra, slot).wait_send()

        for p in range(cuts):
            for blk in range(3):
                share(blk, 0, me, p, sib).wait_send()
                share(blk, 2, me, p, sib).wait_send()
                if (blk, p) not in ((1, 0), (2, cuts - 1)):
                    share(blk, 1, me, p, cross).wait_send()
            near(1, p).wait_send()
            near(2, p).wait_send()
        onward(1, 0).wait_send()
        onward(2, cuts - 1).wait_send()

    margin()

    terms(share_of * bands - 1).wait_send()


def solve(orb, bands, groups, nband, ng):
    width = ng * ng // PTS
    pts, rows = PTS, orb.shape[0] * 128 // (PTS * width)
    step = ng // PTS
    total = pts * width
    xh, xl = split_const(np.kron(hartley(ng), np.eye(bands)))
    hz = np.tile(hartley(ng), (1, 2 * step)).astype(np.float32)
    kt = (kernel_values(ng).astype(np.float32) / np.float32(ng**3)).reshape(ng, total)
    consts = [kt, hz, mixer_rows(ng).astype(np.float32), xh, xl]
    full = (groups, pts, rows, width)
    f32, bf16, dma = jnp.float32, jnp.bfloat16, pltpu.SemaphoreType.DMA
    tall = groups * rows
    xs = rows // bands
    nall, flat = nband * bands, orb.shape[0] // bands
    vmem = pl.BlockSpec(memory_space=pltpu.VMEM)
    return pl.pallas_call(
        functools.partial(solve_kernel, ng),
        out_shape=[pltpu.VMEM(orb.shape, f32), pltpu.VMEM((bands, nall // groups), f32)],
        in_specs=[pl.BlockSpec(memory_space=pltpu.HBM)] * 6,
        out_specs=[vmem] * 2,
        scratch_shapes=[
            pltpu.VMEM(orb.shape, f32), *[pltpu.VMEM(c.shape, c.dtype) for c in consts],
            pltpu.VMEM((3,) + full, f32), pltpu.VMEM(full, f32),
            pltpu.VMEM((groups, width // 128, pts * rows, 128), f32),
            pltpu.VMEM((tall, total), bf16), pltpu.VMEM((tall, total), bf16),
            pltpu.VMEM((tall, total), bf16), pltpu.VMEM((tall, total), bf16),
            pltpu.VMEM((tall, total), f32),
            pltpu.VMEM((2, total, 2 * width), bf16), pltpu.VMEM((2, total, 2 * width), bf16),
            pltpu.VMEM((tall, total), f32),
            pltpu.VMEM((groups, flat, 128), f32), pltpu.VMEM((groups, flat, 128), f32),
            pltpu.VMEM((2, bands, flat, 128), f32), pltpu.VMEM((width // 128, pts * rows, 128), f32),
            pltpu.VMEM((2, nall, 8, 128), f32), pltpu.VMEM((2, nall // 2, 8, 128), f32),
            pltpu.VMEM((2, nall, 1024), bf16), pltpu.VMEM((2, nall, 1024), bf16),
            pltpu.VMEM((nall // 2, nall), f32),
            pltpu.VMEM((nall // 2, 1, nall), f32), pltpu.VMEM((nall // 2, 1, nall), f32),
            dma((3, groups, 3)), dma((3, 3, 3)), dma((2, 3)), dma((2,)), dma((groups,)), dma((groups,)),
            dma((2,)), dma((2, groups)), dma((2,)), dma((2,)),
            dma(()), dma(()), dma((6,)),
        ],
        compiler_params=pltpu.CompilerParams(
            vmem_limit_bytes=56 * 1024 * 1024, collective_id=0, has_side_effects=True
        ),
        cost_estimate=pl.CostEstimate(flops=10**11, bytes_accessed=10**7, transcendentals=0),
        name="solve",
    )(orb, *[jnp.asarray(c) for c in consts])


def on_device(orbitals):
    groups = lax.axis_size("grid")
    bands, local = orbitals.shape
    ncell = local * groups
    ng = round(ncell ** (1 / 3))
    raw = orbitals.reshape(bands, local // 128, 128).transpose(1, 0, 2).reshape(bands * local // 128, 128)
    out, margin = solve(raw, bands, groups, lax.axis_size("band"), ng)
    vectors = out.reshape(local // 128, bands, 128).transpose(1, 0, 2).reshape(bands, local)
    return (vectors, margin.T)


def solution(mesh):
    return jax.shard_map(
        on_device,
        mesh=mesh,
        in_specs=(P("band", "grid"),),
        out_specs=(P("band", "grid"), P("grid", "band")),
        check_vma=False,
    )
```

```python
import functools

import jax
import jax.numpy as jnp
import numpy as np
from jax import lax
from jax.experimental import pallas as pl
from jax.experimental.pallas import tpu as pltpu
from jax.sharding import PartitionSpec as P


PTS = 6


def freq_order(ng):
    step = ng // PTS
    low = np.arange(step) * PTS
    out = [low, low + 3]
    for k in (1, 2):
        out += [low + k, ng - low - k]
    return np.concatenate(out)


def kernel_values(ng):
    freqs = ((np.arange(ng) + ng // 2) % ng - ng // 2).astype(np.float32)
    fy = freqs[freq_order(ng)]
    sq = freqs[:, None, None] ** 2 + fy[None, :, None] ** 2 + freqs[None, None, :] ** 2
    safe = np.where(sq > 0, sq, np.float32(1.0))
    return np.where(sq > 0, 40.0 * (1.0 - np.exp(-sq / 16.0)) / safe, 0.0)


def cas(ang):
    return np.cos(ang) + np.sin(ang)


def hartley(ng):
    k = np.arange(ng)
    return cas((k[:, None] * k[None, :] % ng) * (2.0 * np.pi / ng))


def mixers(ng):
    step = ng // PTS
    s, k2 = np.arange(step)[:, None], np.arange(step)[None, :]
    out = []
    for k1 in (0, 3, 1, 2):
        ang = s * (k1 + PTS * k2) * (2.0 * np.pi / ng)
        p, m = cas(ang), cas(-ang)
        out.append(p if k1 in (0, 3) else np.block([[p, m], [m, -p]]))
    return out


def mixer_rows(ng):
    step = ng // PTS
    fwd, inv = [], []
    for mat in mixers(ng):
        for rows, keep in ((mat, fwd), (mat.T, inv)):
            wide = np.zeros((rows.shape[0], 2 * step))
            wide[:, : rows.shape[1]] = rows
            keep.append(np.repeat(wide, ng, axis=1))
    return np.stack([np.concatenate(fwd), np.concatenate(inv)])


def split_const(table):
    table = np.asarray(table, np.float32)
    hi = table.astype(jnp.bfloat16)
    lo = (table - hi.astype(np.float32)).astype(jnp.bfloat16)
    return hi, lo


def split(v):
    hi = v.astype(jnp.bfloat16)
    lo = (v - hi.astype(jnp.float32)).astype(jnp.bfloat16)
    return hi, lo


def mm(a, b):
    return jnp.dot(a, b, preferred_element_type=jnp.float32)


def solve_kernel(ng, orb_in, kt_in, hz_in, mix_in, xh_in, xl_in, o_ref, m_ref,
                 orb_ref, kt_ref, hz_ref, mix_ref, xh_ref, xl_ref,
                 buf, amp, acc, ch, cl, zh, zl, cb, wh, wl, kx, vec, recv,
                 ox, st, ro, rv, xo, xv, ga, gs, gr,
                 rsem, ssem, nsem, fsem, osem, orsem, so, sv, qo, qv, sg, qg, ls):
    pts, rows, width = buf.shape[2:]
    bands, step = 4, ng // PTS
    xs = rows // bands
    total = pts * width
    me = lax.axis_index("grid")
    band, nband = lax.axis_index("band"), lax.axis_size("band")
    chip, core = me // 2, me % 2
    sib = chip * 2 + (1 - core)
    cross = (1 - chip) * 2 + core
    far = (1 - chip) * 2 + (1 - core)
    above, below = (band + 1) % nband, (band + nband - 1) % nband
    mesh_id = pl.DeviceIdType.MESH
    root = np.float32(np.sqrt(0.75))
    cuts = 3
    per = pts // cuts

    def remote(src, dst, send, recv_sem, device):
        return pltpu.make_async_remote_copy(
            src_ref=src, dst_ref=dst, send_sem=send, recv_sem=recv_sem,
            device_id=device, device_id_type=mesh_id,
        )

    def share(blk, lane, slot, p, target):
        piece = buf.at[blk, slot, pl.ds(per * p, per)]
        return remote(piece, piece, ssem.at[blk, lane, p], rsem.at[blk, slot, p], (band, target))

    def near(blk, p):
        at = pl.ds(per * p, per)
        device = (above if blk == 1 else below, cross)
        return remote(buf.at[0, me, at], buf.at[blk, me, at], nsem.at[blk - 1, p], rsem.at[blk, me, p], device)

    def onward(blk, p):
        at = pl.ds(per * p, per)
        device = (above if blk == 1 else below, cross)
        return remote(buf.at[0, cross, at], buf.at[blk, cross, at], fsem.at[blk - 1], rsem.at[blk, cross, p], device)

    def each(n, body):
        def one(k, _):
            body(k)
            return 0

        lax.fori_loop(0, n, one, 0)


    lanes = width // 128
    tile, nall = 8, nband * bands
    yy, zz, xh = band % 8 // 2, band // 8, band % 2
    moves = ((0, 0), (1, 0), (3, 0), (0, 1), (0, 3), (1, 1), (1, 3), (2, 0))
    share_of = 2 * len(moves)
    extra = pts * xs * lanes // tile - share_of

    def base(y, z):
        return z % 4 * 8 + y % 4 * 2

    def shade(y, z):
        return (y + z // 2 * 2) % 4 + z % 2 * 4

    targets = [(base(yy + oy, zz + oz), shade((yy + oy) % 4, (zz + oz) % 4)) for oy, oz in moves]
    sources = [base(yy + 4 - oy, zz + 4 - oz) for oy, oz in moves]
    double = shade(yy, zz) + 8 * xh < extra

    def tile_at(t):
        return pl.ds(pl.multiple_of(t * tile, tile), tile)

    def send_orb(src, b):
        mine = pl.ds(b * bands, bands)

        def one(e, y, z, k):
            home = jnp.logical_and(yy == y, zz == z)
            at = tile_at(e + 8 * xh + share_of * k)

            @pl.when(jnp.logical_not(home))
            def _():
                remote(src.at[:, at], ro.at[k, mine], so.at[k], qo.at[k], (base(y, z) + xh, me)).start()

            @pl.when(home)
            def _():
                ro[k, mine] = src[:, at]

        for e in range(8):
            for w in range(2):
                y, z = (e % 4 + 2 * w) % 4, e // 4 + 2 * w
                one(e, y, z, 0)
                if e + 8 < extra:
                    one(e, y, z, 1)
                else:
                    @pl.when(xh == 0)
                    def _():
                        one(e, y, z, 1)

    def orbs(k, n):
        piece = ro.at[k, pl.ds(0, bands * n)]
        return remote(piece, piece, so.at[k], qo.at[k], (band, sib))

    def send_vec(slot):
        def one(i, x, k):
            where, q = targets[i]
            t = q + 8 * x + share_of * k
            index = (i * 2 + xh) * bands + me

            def go():
                remote(vec.at[slot, tile_at(t)], rv.at[k, index], sv.at[k, slot], qv.at[k], (where + x, slot)).start()

            if i > 0:
                go()
                return
            home = jnp.logical_and(xh == x, slot == me)
            pl.when(jnp.logical_not(home))(go)

            @pl.when(home)
            def _():
                rv[k, index] = vec[slot, tile_at(t)]

        for i in range(len(moves) - 1, -1, -1):
            for x in range(2):
                one(i, x, 0)
                if x == 0:
                    one(i, x, 1)
                else:
                    @pl.when(targets[i][1] + 8 < extra)
                    def _():
                        one(i, x, 1)

    def vecs(k, n, slot):
        piece = rv.at[k, pl.ds(0, n)]
        return remote(piece, piece, sv.at[k, slot], qv.at[k], (band, sib))

    def lay_orb():
        for r in range(pts):
            for j in range(lanes):
                for b in range(bands):
                    first = bands * (lanes * r + j) + b
                    rows_b = orb_ref[pl.ds(first, xs, stride=pts * lanes * bands), :]
                    ox[0, b, pts * xs * j + xs * r : pts * xs * j + xs * r + xs, :] = rows_b

    def lay_mate():
        blk = 2 - xh
        for j in range(lanes):
            for r in range(pts):
                st[j, rows * r : rows * r + rows, :] = buf[blk, me, r, :, 128 * j : 128 * j + 128]
            for b in range(bands):
                ox[1, b, pts * xs * j : pts * xs * (j + 1), :] = st[j, pl.ds(b, pts * xs, stride=bands), :]

    def term(m, g):
        return remote(gs.at[m * bands + g], gr.at[(m // 2 * 2 + xh) * bands + me], sg, qg, (sources[m // 2] + m % 2, g))

    def terms(n):
        return remote(gs.at[pl.ds(0, n)], gs.at[pl.ds(0, n)], sg, qg, (band, sib))

    def send_terms():
        for m in range(share_of - 1, -1, -1):
            for g in range(bands):
                if m > 1:
                    term(m, g).start()
                else:
                    home = jnp.logical_and(xh == m, me == g)

                    @pl.when(jnp.logical_not(home))
                    def _():
                        term(m, g).start()

                    @pl.when(home)
                    def _():
                        gr[xh * bands + me] = gs[m * bands + g]

    def regroup(g):
        sub = lax.broadcasted_iota(jnp.int32, g.shape, 0) % bands
        quarter = nall // bands
        lane = lax.broadcasted_iota(jnp.int32, g.shape, 1) // quarter
        out = g
        for d in range(1, bands):
            moved = jnp.where(sub >= d, pltpu.roll(g, d, 0), pltpu.roll(g, g.shape[0] + d - bands, 0))
            moved = pltpu.roll(moved, nall - quarter * d, 1)
            out = jnp.where((sub + bands - lane) % bands == d, moved, out)
        return out

    def take(src, n):
        flat = src.reshape(n * tile, 128)
        return split(jnp.concatenate([flat[pl.ds(r, n, stride=tile), :] for r in range(tile)], axis=1))

    def nt(a, b):
        return lax.dot_general(a, b, (((1,), (1,)), ((), ())), preferred_element_type=jnp.float32)

    barrier = pltpu.get_barrier_semaphore()
    def greet(device):
        pl.semaphore_signal(barrier, inc=1, device_id=device, device_id_type=mesh_id)

    for device in ((band, sib), (band, cross), (band, far), (above, cross), (below, cross)):
        greet(device)
    each(nband - 1, lambda k: greet((jnp.where(k >= band, k + 1, k), me)))
    pairs = ((orb_in, orb_ref), (hz_in, hz_ref), (mix_in, mix_ref), (kt_in, kt_ref), (xh_in, xh_ref), (xl_in, xl_ref))
    loads = [pltpu.make_async_copy(src, dst, ls.at[n]) for n, (src, dst) in enumerate(pairs)]
    for load in loads:
        load.start()
    loads[0].wait()

    def lay_own(q):
        for h in range(2):
            for r in range(pts):
                for j in range(width // 128):
                    unit = ((2 * q + h) * pts + r) * (width // 128) + j
                    piece = orb_ref[bands * unit : bands * unit + bands, :]
                    at = (me, r, pl.ds(8 * q + 4 * h, bands), pl.ds(128 * j, 128))
                    buf[(0,) + at] = piece

    for q in range(xs // 2):
        lay_own(q)
    pl.semaphore_wait(barrier, nband + 4)

    for p in range(cuts):
        share(0, 1, me, p, cross).start()
    for p in range(cuts):
        share(0, 0, me, p, sib).start()
    for p in range(cuts):
        near(1, p).start()

    def weights(first, last, cols):
        def one(u, _):
            at = pl.ds(pl.multiple_of(u * ng, 16), ng)
            for d in range(2):
                hi, lo = split(hz_ref[:, :cols] * mix_ref[d, pl.ds(u, 1), :cols])
                wh[d, at, :cols] = hi
                wl[d, at, :cols] = lo
            return 0

        lax.fori_loop(first, last, one, 0)

    for load in loads[1:]:
        load.wait()
    weights(0, 2 * step, width)
    weights(2 * step, PTS * step, 2 * width)

    def spread_rows(t):
        upper = lax.broadcasted_iota(jnp.int32, (8, total), 0) < 4
        a = jnp.broadcast_to(kt_ref[pl.ds(2 * t, 1), :], (8, total))
        b = jnp.broadcast_to(kt_ref[pl.ds(2 * t + 1, 1), :], (8, total))
        kx[pl.ds(pl.multiple_of(8 * t, 8), 8), :] = jnp.where(upper, a, b)

    each(ng // 2, spread_rows)
    lay_orb()

    def arrived(blk, slot, p):
        share(blk, 0, slot, p, sib).wait_recv()

    def relay(blk, slot, p):
        arrived(blk, slot, p)
        share(blk, 2, slot, p, sib).start()

    def spread(blk, p, wide):
        arrived(blk, cross, p)
        if wide:
            share(blk, 1, cross, p, cross).start()
        share(blk, 0, cross, p, sib).start()

    def slot_of(blk, s):
        turn = s // 2 + jnp.minimum(blk, 1)
        return ((chip + turn) % 2) * 2 + (core + s % 2) % 2

    def amplitude(slot):
        sub = lax.broadcasted_iota(jnp.int32, (8, 128), 0)
        pick = sub // bands * bands + me

        def one(r):
            for q in range(rows // 8):
                for j in range(width // 128):
                    at = (slot, r, pl.ds(8 * q, 8), pl.ds(128 * j, 128))
                    amp[at] = jnp.take_along_axis(buf[(0,) + at], pick, axis=0)

        each(pts, one)

    def pieces():
        for q in range(rows // 16):
            for j in range(width // 128):
                yield q, j

    def forward(blk, s):
        slot = slot_of(blk, s)

        @pl.when(jnp.logical_and(blk == 0, s == 2))
        def _():
            for p in range(cuts):
                relay(0, cross, p)
                if p == 0:
                    near(2, 0).start()
                    onward(1, 0).start()
                    for k in range(1, cuts):
                        near(2, k).start()
                if p == cuts - 1:
                    onward(2, p).start()
                spread(1, p, p > 0)

        @pl.when(s % 2 == 1)
        def _():
            for p in range(cuts):
                arrived(blk, slot, p)

        @pl.when(blk == 0)
        def _():
            amplitude(slot)

        for q, j in pieces():
            at = (pl.ds(16 * q, 16), pl.ds(128 * j, 128))
            f = [amp[(slot, r) + at] * buf[(blk, slot, r) + at] for r in range(PTS)]
            sa, sb, sc = f[0] + f[3], f[1] + f[4], f[2] + f[5]
            da, db, dc = f[0] - f[3], f[1] - f[4], f[2] - f[5]
            even, odd = sb + sc, db - dc
            comps = (sa + even, da - odd, da + 0.5 * odd, root * (db + dc), sa - 0.5 * even, root * (sb - sc))
            to = pl.ds(pl.multiple_of(slot * rows + 16 * q, 16), 16)
            for c, v in enumerate(comps):
                hi, lo = split(v)
                ch[to, c * width + 128 * j : c * width + 128 * j + 128] = hi
                cl[to, c * width + 128 * j : c * width + 128 * j + 128] = lo

    groups = ((0, 1), (1, 1), (2, 2), (4, 2))

    def planar(d, ah, al, emit, at):
        for first, count in groups:
            lo, size = first * width, count * width
            for n in range(0, size, 256):
                w = min(256, size - n)
                a, b = ah[at, lo : lo + size], al[at, lo : lo + size]
                g, h = wh[d, lo : lo + size, n : n + w], wl[d, lo : lo + size, n : n + w]
                emit(at, slice(lo + n, lo + n + w), mm(a, g) + mm(b, g) + mm(a, h))

    def keep_split(at, to, v):
        zh[at, to], zl[at, to] = split(v)

    def keep(at, to, v):
        cb[at, to] = v

    def xpass(h, l):
        return mm(xh_ref[...], h) + mm(xh_ref[...], l) + mm(xl_ref[...], h)

    def xconv():
        for n in range(0, total, 256):
            h, l = split(xpass(zh[:, n : n + 256], zl[:, n : n + 256]) * kx[:, n : n + 256])
            zh[:, n : n + 256], zl[:, n : n + 256] = split(xpass(h, l))

    def push(slot):
        return remote(vec.at[slot], recv.at[me], osem.at[slot], orsem.at[me], (band, slot))

    def inverse(blk, s):
        slot = ((chip + 1 - s // 2) % 2) * 2 + (core + s % 2 + s // 2) % 2
        fresh = blk == 0
        for q, j in pieces():
            to = pl.ds(pl.multiple_of(slot * rows + 16 * q, 16), 16)
            c0, c3, c1, s1, c2, s2 = [cb[to, c * width + 128 * j : c * width + 128 * j + 128] for c in range(PTS)]
            ea, eb, oa, ob = c0 - 0.5 * c2, root * s2, c3 - 0.5 * c1, root * s1
            even = (c0 + c2, ea + eb, ea - eb)
            odd = (c3 + c1, ob - oa, oa + ob)
            for r in range(PTS):
                v = even[r % 3] + odd[r % 3] if r < 3 else even[r % 3] - odd[r % 3]
                w = v * buf[blk, slot, r, 16 * q : 16 * q + 16, 128 * j : 128 * j + 128]
                at = (slot, j, pl.ds(rows * r + 16 * q, 16))
                acc[at] = jnp.where(fresh, w, acc[at] + w)

        @pl.when(blk == 2)
        def _():
            for j in range(width // 128):
                t = [acc[slot, j, pl.ds(b, pts * xs, stride=bands), :] for b in range(bands)]
                vec[slot, pts * xs * j : pts * xs * (j + 1), :] = -((t[0] + t[1]) + (t[2] + t[3]))

            send_vec(slot)

    def product(k):
        vh, vl = take(rv.at[k], share_of * bands)
        return nt(vh, xo[k]) + nt(vh, xv[k]) + nt(vl, xo[k])

    def margin():
        others = 2 * (nband // 2 - 1)
        orbs(0, others).wait_recv()
        xo[0], xv[0] = take(ro.at[0], nall)

        @pl.when(double)
        def _():
            orbs(1, others).wait_recv()
            xo[1], xv[1] = take(ro.at[1], nall)

        vecs(0, share_of * bands - 1, 0).wait_recv()
        ga[...] = product(0)

        @pl.when(double)
        def _():
            vecs(1, share_of * bands - 1, 0).wait_recv()
            ga[...] += product(1)

        g = regroup(ga[...])
        for n in range(share_of * bands):
            gs[n] = g[n : n + 1]
        send_terms()
        drain()
        held = share_of * bands
        terms(held - 1).wait_recv()
        collect()
        sums = [gr[n] for n in range(4)]
        for n in range(4, held):
            sums[n % 4] += gr[n]
        full = ((sums[0] + sums[1]) + (sums[2] + sums[3])) * (1.0 / ng**3)
        for k in range(bands):
            m_ref[k : k + 1, :] = full[:, k * m_ref.shape[1] : (k + 1) * m_ref.shape[1]]

    def block(blk):
        def half(h):
            forward(blk, 2 * h)
            forward(blk, 2 * h + 1)
            which = (chip + jnp.minimum(blk, 1) + h) % 2
            planar(0, ch, cl, keep_split, pl.ds(pl.multiple_of(which * 2 * rows, 32), 2 * rows))

        @pl.when(blk < 2)
        def _():
            each(2, half)

        @pl.when(blk == 2)
        def _():
            each(4, lambda s: forward(blk, s))
            planar(0, ch, cl, keep_split, slice(None))


        @pl.when(blk == 1)
        def _():
            spread(2, 1, True)

        xconv()

        @pl.when(blk == 0)
        def _():
            spread(2, 0, True)

        @pl.when(blk == 1)
        def _():
            spread(2, 2, False)
            send_orb(ox.at[0], band)

        planar(1, zh, zl, keep, slice(None))

        @pl.when(blk == 0)
        def _():
            for p in range(cuts):
                relay(1, me, p)

        @pl.when(blk == 1)
        def _():
            for p in range(cuts):
                relay(2, me, p)
            lay_mate()
            send_orb(ox.at[1], band + 1 - 2 * xh)

        each(4, lambda s: inverse(blk, s))

    each(3, block)

    def place(slot, src):
        for r in range(pts):
            for j in range(width // 128):
                piece = src[pts * xs * j + xs * r : pts * xs * j + xs * r + xs, :]
                o_ref[pl.ds(bands * (width // 128 * r + j) + slot, xs, stride=pts * width // 128 * bands), :] = piece

    for slot in (cross, far, sib):
        push(slot).start()

    def collect():
        recv[me] = vec[me]
        for slot in (sib, cross, far):
            remote(vec.at[slot], recv.at[slot], osem.at[slot], orsem.at[slot], (band, slot)).wait()
        for k in range(4):
            place(k, recv[k])

    def drain():
        orbs(0, 2 * (nband // 2 - 1)).wait_send()
        few = 4 * (extra - 8)

        @pl.when(xh == 0)
        def _():
            orbs(1, 2 * (nband // 2 - 1)).wait_send()

        @pl.when(jnp.logical_and(xh == 1, double))
        def _():
            orbs(1, few - 2).wait_send()

        @pl.when(jnp.logical_and(xh == 1, jnp.logical_not(double)))
        def _():
            orbs(1, few).wait_send()

        for slot in range(4):
            @pl.when(me == slot)
            def _():
                vecs(0, share_of - 1, slot).wait_send()

            @pl.when(me != slot)
            def _():
                vecs(0, share_of, slot).wait_send()

            home = jnp.logical_and(double, me == slot)

            @pl.when(home)
            def _():
                vecs(1, extra - 1, slot).wait_send()

            @pl.when(jnp.logical_not(home))
            def _():
                vecs(1, extra, slot).wait_send()

        for p in range(cuts):
            for blk in range(3):
                share(blk, 0, me, p, sib).wait_send()
                share(blk, 2, me, p, sib).wait_send()
                if (blk, p) not in ((1, 0), (2, cuts - 1)):
                    share(blk, 1, me, p, cross).wait_send()
            near(1, p).wait_send()
            near(2, p).wait_send()
        onward(1, 0).wait_send()
        onward(2, cuts - 1).wait_send()

    margin()

    terms(share_of * bands - 1).wait_send()


def solve(orb, bands, groups, nband, ng):
    width = ng * ng // PTS
    pts, rows = PTS, orb.shape[0] * 128 // (PTS * width)
    step = ng // PTS
    total = pts * width
    xh, xl = split_const(np.kron(hartley(ng), np.eye(bands)))
    hz = np.tile(hartley(ng), (1, 2 * step)).astype(np.float32)
    kt = (kernel_values(ng).astype(np.float32) / np.float32(ng**3)).reshape(ng, total)
    consts = [kt, hz, mixer_rows(ng).astype(np.float32), xh, xl]
    full = (groups, pts, rows, width)
    f32, bf16, dma = jnp.float32, jnp.bfloat16, pltpu.SemaphoreType.DMA
    tall = groups * rows
    xs = rows // bands
    nall, flat = nband * bands, orb.shape[0] // bands
    vmem = pl.BlockSpec(memory_space=pltpu.VMEM)
    return pl.pallas_call(
        functools.partial(solve_kernel, ng),
        out_shape=[pltpu.VMEM(orb.shape, f32), pltpu.VMEM((bands, nall // groups), f32)],
        in_specs=[pl.BlockSpec(memory_space=pltpu.HBM)] * 6,
        out_specs=[vmem] * 2,
        scratch_shapes=[
            pltpu.VMEM(orb.shape, f32), *[pltpu.VMEM(c.shape, c.dtype) for c in consts],
            pltpu.VMEM((3,) + full, f32), pltpu.VMEM(full, f32),
            pltpu.VMEM((groups, width // 128, pts * rows, 128), f32),
            pltpu.VMEM((tall, total), bf16), pltpu.VMEM((tall, total), bf16),
            pltpu.VMEM((tall, total), bf16), pltpu.VMEM((tall, total), bf16),
            pltpu.VMEM((tall, total), f32),
            pltpu.VMEM((2, total, 2 * width), bf16), pltpu.VMEM((2, total, 2 * width), bf16),
            pltpu.VMEM((tall, total), f32),
            pltpu.VMEM((groups, flat, 128), f32), pltpu.VMEM((groups, flat, 128), f32),
            pltpu.VMEM((2, bands, flat, 128), f32), pltpu.VMEM((width // 128, pts * rows, 128), f32),
            pltpu.VMEM((2, nall, 8, 128), f32), pltpu.VMEM((2, nall // 2, 8, 128), f32),
            pltpu.VMEM((2, nall, 1024), bf16), pltpu.VMEM((2, nall, 1024), bf16),
            pltpu.VMEM((nall // 2, nall), f32),
            pltpu.VMEM((nall // 2, 1, nall), f32), pltpu.VMEM((nall // 2, 1, nall), f32),
            dma((3, groups, 3)), dma((3, 3, 3)), dma((2, 3)), dma((2,)), dma((groups,)), dma((groups,)),
            dma((2,)), dma((2, groups)), dma((2,)), dma((2,)),
            dma(()), dma(()), dma((6,)),
        ],
        compiler_params=pltpu.CompilerParams(
            vmem_limit_bytes=56 * 1024 * 1024, collective_id=0, has_side_effects=True
        ),
        cost_estimate=pl.CostEstimate(flops=10**11, bytes_accessed=10**7, transcendentals=0),
        name="solve",
    )(orb, *[jnp.asarray(c) for c in consts])


def on_device(orbitals):
    groups = lax.axis_size("grid")
    bands, local = orbitals.shape
    ncell = local * groups
    ng = round(ncell ** (1 / 3))
    raw = orbitals.reshape(bands, local // 128, 128).transpose(1, 0, 2).reshape(bands * local // 128, 128)
    out, margin = solve(raw, bands, groups, lax.axis_size("band"), ng)
    vectors = out.reshape(local // 128, bands, 128).transpose(1, 0, 2).reshape(bands, local)
    return (vectors, margin.T)


def solution(mesh):
    return jax.shard_map(
        on_device,
        mesh=mesh,
        in_specs=(P("band", "grid"),),
        out_specs=(P("band", "grid"), P("grid", "band")),
        check_vma=False,
    )
```
